256 devices in a mesh: seq: 32 (over z, y), vocab: 8 (over x, core).
Axes of the slice: x: 4, y: 4, z: 8, core: 2. Of those that a mesh axis runs over, the one named last changes fastest.
Arguments:
- hidden: bfloat16 [3072, 3584], P('seq', 'vocab'), may hold values from -40 to 40
- lm_head: bfloat16 [3584, 152064], P(None, ('seq', 'vocab')), may hold values from -1 to 1
- positions: int32 [3072], replicated, may hold values from 0 to 3071, as said below
- vocab_limits: int32 [3072], replicated, may hold values from 76032 to 152064
- loss_mask: int32 [3072], P('seq'), may hold values 0 or 1
Outputs:
- token_entropy: float32 [3072], P('seq')
- mean_entropy: float32 [], replicated
The draws below stay inside these ranges and needn't reach their ends.
Inputs may be any that keep to these rules, and one draw needn't show every extreme that they name: A permutation of the positions 0 to 3071: the response is cut into 64 blocks of 48 consecutive positions; rows i * 96 to i * 96 + 96 // 2 - 1 hold the positions of block i, the next 48 rows those of block 63 - i, in any order within a block.
All inputs are finite; a program needn't handle non-finite values. No bound on the sum of `loss_mask` on one device may be relied on, other than what follows from the above.
Results may differ from the reference program's by a relative error of at most 0.0003.
Values may be sent and summed in bfloat16 or wider, within the bound.
A program may use at most 128 MiB of HBM per device.

```python
import math
import jax
import jax.numpy as jnp
from jax import lax

D = 3584
VOCAB = 152064
TOK_DEV = 96
TOKENS = 3072


def shared_weights(key):
    return jax.random.normal(jax.random.fold_in(key, 11), (D, VOCAB), jnp.float32) / math.sqrt(D)


def draw_lm_head(key, part):
    return shared_weights(key).astype(jnp.bfloat16)


def draw_positions(key, part):
    groups = TOKENS // TOK_DEV
    half = TOK_DEV // 2
    block_keys = jax.random.split(jax.random.fold_in(key, 21), 2 * groups)
    inner = jax.vmap(lambda one_key: jax.random.permutation(one_key, half))(block_keys).astype(jnp.int32)
    first_block = jnp.arange(groups, dtype=jnp.int32)
    second_block = 2 * groups - 1 - first_block
    rows = jnp.stack([first_block[:, None] * half + inner[first_block], second_block[:, None] * half + inner[second_block]], axis=1)
    return rows.reshape(TOKENS).astype(jnp.int32)


def draw_hidden(key, part):
    values = 3.0 * jax.random.normal(jax.random.fold_in(key, 12), (TOKENS, D), jnp.float32)
    return jnp.clip(values, -40.0, 40.0).astype(jnp.bfloat16)


def touch_ends(drawn, rng, least, largest):
    shape = drawn.shape
    place = [jax.random.randint(jax.random.fold_in(rng, axis), (), 0, shape[axis]) for axis in range(len(shape))]
    drawn = drawn.at[tuple(place)].set(least)
    longest = shape.index(max(shape))
    place[longest] = (place[longest] + 1) % shape[longest]
    return drawn.at[tuple(place)].set(largest)


def setup_inputs(seed: int = 0) -> dict:
    key_of = jax.random.split(jax.random.key(seed), 6)
    return {
        "hidden": draw_hidden(jax.random.fold_in(key_of[5], 71), 0),
        "lm_head": draw_lm_head(jax.random.fold_in(key_of[5], 71), 0),
        "positions": draw_positions(jax.random.fold_in(key_of[5], 71), 0),
        "vocab_limits": touch_ends(jax.random.randint(key_of[3], (TOKENS,), VOCAB // 2, VOCAB + 1), jax.random.fold_in(key_of[3], 1), VOCAB // 2, VOCAB).astype(jnp.int32),
        "loss_mask": touch_ends((jax.random.randint(key_of[4], (TOKENS,), 0, 4) < 3).astype(jnp.int32), jax.random.fold_in(key_of[4], 1), 0, 1),
    }


masked_value = -1e30


def row_stats(logits, row_limits, first_column):
    columns = first_column + lax.iota(jnp.int32, logits.shape[1])
    allowed = columns[None, :] < row_limits[:, None]
    row_peak = jnp.max(jnp.where(allowed, logits, masked_value), axis=1)
    shifted = logits - row_peak[:, None]
    weights = jnp.where(allowed, jnp.exp(shifted), 0.0)
    row_total = jnp.sum(weights, axis=1)
    row_moment = jnp.sum(weights * jnp.where(allowed, shifted, 0.0), axis=1)
    return row_peak, row_total, row_moment


def reference(hidden, lm_head, positions, vocab_limits, loss_mask):
    def block_entropy(inputs):
        block_rows, limits_here = inputs
        logits = jnp.dot(block_rows, lm_head, preferred_element_type=jnp.float32)
        row_peak, row_total, row_moment = row_stats(logits, limits_here, 0)
        return jnp.log(row_total) - row_moment / row_total

    entropy_rows = lax.map(block_entropy, (hidden.reshape(-1, TOK_DEV, D), vocab_limits.reshape(-1, TOK_DEV)))
    token_entropy = jnp.zeros((TOKENS,), jnp.float32).at[positions].set(entropy_rows.reshape(-1))
    mask_float = loss_mask.astype(jnp.float32)
    mean_entropy = jnp.sum(token_entropy * mask_float) / jnp.maximum(jnp.sum(mask_float), 1.0)
    return token_entropy, mean_entropy
```

```python
import heapq

import jax
import jax.numpy as jnp
from jax import lax
from jax.experimental import pallas as pl
from jax.experimental.pallas import tpu as pltpu
from jax.sharding import Mesh
from jax.sharding import PartitionSpec as P

NZ, NY, NX = 8, 4, 4
SIZE = {"z": NZ, "y": NY, "x": NX}
AXES = ("z", "y", "x", "c")
MESH = pl.DeviceIdType.MESH
HALF, RB, COLORS = 48, 16, 3
TOK = 96
ROWS = NY * HALF
D, FEAT = 3584, 896
WID, SLOT = 594, 640
COLS = 2 * SLOT
TILE = 256
NEG = -1e30
ORDER = (0, 1, 7, 2, 6, 3, 5, 4)
DEADLINE = (8.7, 7.5, 14.8, 17.9, 19.6)
UNIT, HOP, BACKLOG = 0.615, 1.75, 2.0
WINDOW = 2.9


def onward(n, d, far):
    if d == 0:
        return [1, -1]
    if d < n // 2:
        return [-1] if d + 1 < n // 2 or far == -1 else []
    if d > n // 2:
        return [1] if d - 1 > n // 2 or far == 1 else []
    return []


def parity(k):
    return 1 if k % 2 == 0 else -1


def sends_of(p):
    color, axis, rest = p[0], p[1], p[2:]
    out = []
    if color == "A" and axis == "y":
        (dy,) = rest
        out += [("y", m, 1, ("A", "y", (dy - m) % 4)) for m in onward(4, dy, 1)]
        out += [("x", m, 1, ("A", "x", dy, -m % 4)) for m in (1, -1)]
    elif color == "A" and axis == "x":
        dy, dx = rest
        out += [("x", m, 1, ("A", "x", dy, (dx - m) % 4)) for m in onward(4, dx, parity(dy))]
    elif color == "A":
        dz, dy = rest
        out += [("z", m, 4, ("A", "z", (dz - m) % 8, dy)) for m in onward(8, dz, parity(dy))]
    elif axis == "z":
        (dz,) = rest
        far = 1 if color == "B" else -1
        out += [("z", m, 1, (color, "z", (dz - m) % 8)) for m in onward(8, dz, far)]
        second = "y" if color == "B" else "x"
        out += [(second, m, 1, (color, second, dz, -m % 4)) for m in (1, -1)]
    else:
        dz, d = rest
        last = (color, axis) in (("B", "x"), ("C", "y"))
        size = 4 if last else 1
        out += [(axis, m, size, (color, axis, dz, (d - m) % 4)) for m in onward(4, d, parity(dz))]
    return out


def launch_of(p):
    color, axis = p[0], p[1]
    if color == "A" and axis != "z":
        return ("A", "z", 0, p[2])
    if color == "B" and axis != "x":
        return ("B", "x", p[2], 0)
    if color == "C" and axis != "y":
        return ("C", "y", p[2], 0)
    return None


def parts_of(launch):
    color, _, a, b = launch
    if color == "A":
        return [("A", "y", b)] + [("A", "x", b, k) for k in (1, 2, 3)]
    if color == "B":
        return [("B", "z", a)] + [("B", "y", a, k) for k in (1, 2, 3)]
    return [("C", "z", a)] + [("C", "x", a, k) for k in (1, 2, 3)]


def window_of(p):
    return 0 if p[0] == "A" and p[1] != "z" else p[2]


def pieces_of_window(dz):
    need = [("B", "x", dz, k) for k in range(4)] + [("C", "y", dz, k) for k in range(4)]
    return need + [("A", "z", dz, k) for k in range(4)]


def plan(preps):
    due = {}

    def latest(p):
        if p not in due:
            dz = window_of(p)
            k = DEADLINE[min(dz, 8 - dz)]
            ahead = sends_of(p)
            launch = launch_of(p)
            if launch:
                ahead = ahead + sends_of(launch)
            for _, _, size, q in ahead:
                k = min(k, latest(q) - HOP - size * UNIT - 0.3)
            due[p] = k
        return due[p]

    free = {(a, m): 0.0 for a in "xyz" for m in (1, -1)}
    waiting = {k: [] for k in free}
    have, steps, flying = set(), [], []
    count = 0
    now = 0.0

    def offer(sends):
        nonlocal count
        for axis, m, size, q in sends:
            heapq.heappush(waiting[axis, m], (latest(q) - size * UNIT, count, size, q))
            count += 1

    def pump():
        nonlocal count
        for link in free:
            while waiting[link] and free[link] - now < BACKLOG:
                _, _, size, q = heapq.heappop(waiting[link])
                free[link] = max(free[link], now) + size * UNIT
                heapq.heappush(flying, (free[link] + HOP, count, q))
                count += 1
                steps.append(("send", link[0], link[1], q))

    def take(p):
        have.add(p)
        offer(sends_of(p))
        launch = launch_of(p)
        if launch and launch not in have and all(q in have for q in parts_of(launch)):
            have.add(launch)
            offer(sends_of(launch))

    for p in (("A", "y", 0), ("B", "z", 0), ("C", "z", 0)):
        take(p)
    pump()
    left = list(ORDER)
    preps = list(preps)
    while flying or left:
        if flying and flying[0][0] <= now:
            _, _, q = heapq.heappop(flying)
            steps.append(("wait", q))
            take(q)
            pump()
            now += 0.03
            continue
        if preps and now >= preps[0][1]:
            name, _, cost = preps.pop(0)
            steps.append(("prep", name))
            now += cost
            pump()
            continue
        ready = [] if preps else [w for w in left if all(q in have for q in pieces_of_window(w))]
        if ready:
            left.remove(ready[0])
            steps.append(("window", ready[0]))
            now += WINDOW
            pump()
            continue
        nxt = [flying[0][0]] if flying else []
        if preps:
            nxt.append(preps[0][1])
        now = max(now, min(nxt))
    return steps


PREPS = (
    [(("limits", k), 0.2, 0.45) for k in range(6)]
    + [(("places", 0), 3.0, 0.4)]
    + [(("own", k), 4.0, 0.3) for k in range(2)]
    + [(("other", k), 11.0, 0.3) for k in range(2)]
    + [(("mask", 0), 12.0, 0.1), (("mask", 1), 17.0, 0.1)]
)
STEPS = plan(PREPS)
TRANSFERS = [s[3] for s in STEPS if s[0] == "send"]
NUMBER = {q: k for k, q in enumerate(TRANSFERS)}


def merge(parts):
    peak = parts[0][0]
    for p in parts[1:]:
        peak = jnp.maximum(peak, p[0])
    total = jnp.zeros_like(peak)
    moment = jnp.zeros_like(peak)
    for m, t, mo in parts:
        shift = m - peak
        ratio = jnp.exp(shift)
        total = total + ratio * t
        moment = moment + ratio * (mo + t * shift)
    return peak, total, moment


def kernel(hid_ref, lm_ref, pos_ref, lim_ref, mask_ref, ent_ref, mean_ref,
           held, weight, stage, hstage, pstage, logits, turned, lim_col, pos_col, cols,
           slab, stat, from_z, plane, from_plane, ents, masks,
           send_sem, recv_sem, hx_sem, w_sem, mz_sem, my_sem, rz_sem, rp_sem, re_sem, copy_sem):
    z, y, x, c = (lax.axis_index(a) for a in AXES)
    here = {"z": z, "y": y, "x": x, "c": c}

    def device(**moved):
        return tuple(lax.rem(here[a] + moved[a], SIZE[a]) if a in moved and a != "c" else
                     (1 - c if a in moved else here[a]) for a in AXES)

    own_w = pltpu.make_async_copy(lm_ref, stage.at[0], copy_sem.at[0])
    own_h = pltpu.make_async_copy(hid_ref, hstage, copy_sem.at[1])
    own_h.start()
    own_w.start()

    barrier = pltpu.get_barrier_semaphore()
    near = [device(**{a: d}) for a in "zyx" for d in (1, SIZE[a] - 1)] + [device(c=1)]
    for who in near:
        pl.semaphore_signal(barrier, inc=1, device_id=who, device_id_type=MESH)
    pl.semaphore_wait(barrier, len(near))

    own_h.wait()
    swap = pltpu.make_async_remote_copy(
        src_ref=hstage.at[pl.ds(pl.multiple_of((1 - c) * HALF, RB), HALF), :], dst_ref=pstage,
        send_sem=hx_sem.at[0], recv_sem=hx_sem.at[1], device_id=device(c=1), device_id_type=MESH)
    swap.start()
    give_w = pltpu.make_async_remote_copy(
        src_ref=lm_ref, dst_ref=stage.at[1],
        send_sem=w_sem.at[0], recv_sem=w_sem.at[1], device_id=device(c=1), device_id_type=MESH)

    def feature(dx):
        return pl.ds(pl.multiple_of(lax.rem(x + dx, NX) * FEAT, 128), FEAT)

    mine = hstage[pl.ds(pl.multiple_of(c * HALF, RB), HALF), :].astype(jnp.float32)
    swap.wait_recv()
    theirs = pstage[...].astype(jnp.float32)
    first = c == 0
    left = jnp.where(first, mine, theirs)
    right = jnp.where(first, theirs, mine)
    both = jnp.concatenate([left, right], axis=1).astype(jnp.bfloat16)
    for k in range(COLORS):
        held[0, 0, k, :, feature(0)] = both[k * RB:(k + 1) * RB]

    def place(p):
        color, axis = p[0], p[1]
        if color == "A":
            if axis == "z":
                return held.at[p[2], p[3], 0]
            return held.at[0, p[2], 0, :, feature(0 if axis == "y" else p[3])]
        if axis == "z":
            return held.at[p[2], 0, 1 if color == "B" else 2, :, feature(0)]
        if color == "B":
            if axis == "y":
                return held.at[p[2], p[3], 1, :, feature(0)]
            return held.at[p[2], :, 1, :, feature(p[3])]
        if axis == "x":
            return held.at[p[2], 0, 2, :, feature(p[3])]
        return held.at[p[2], p[3], 2]

    def transfer(q, axis, m):
        k = NUMBER[q]
        n = SIZE[axis]
        if axis == "x":
            source = q[:-1] + ((q[-1] + m) % n,)
        else:
            at = {("A", "y"): 2, ("A", "z"): 2, ("B", "z"): 2, ("C", "z"): 2}.get(q[:2], 3)
            source = q[:at] + ((q[at] + m) % n,) + q[at + 1:]
        if (q[0], axis) in (("A", "x"), ("B", "y"), ("C", "x")) and source[3] == 0:
            source = (q[0], "y" if q[0] == "A" else "z", q[2])
        dst = place(q)
        if axis == "x":
            src = dst_at = None
            column = feature(q[-1] + m + NX)
            if q[0] == "A":
                src = dst_at = held.at[0, q[2], 0, :, column]
            elif q[0] == "B":
                src = dst_at = held.at[q[2], :, 1, :, column]
            else:
                src = dst_at = held.at[q[2], 0, 2, :, column]
            dst = dst_at
        else:
            src = place(source)
        return pltpu.make_async_remote_copy(
            src_ref=src, dst_ref=dst, send_sem=send_sem.at[k], recv_sem=recv_sem.at[k],
            device_id=device(**{axis: m % n}), device_id_type=MESH)

    started = {}
    lanes = lax.broadcasted_iota(jnp.int32, (128, 128), 1)

    def limits(k):
        if k == 0:
            pad = jnp.zeros((128 - 24, 128), jnp.float32)
            turned[0] = jnp.concatenate([lim_ref[...].astype(jnp.float32), pad], axis=0).T
            turned[1] = jnp.concatenate([pos_ref[...].astype(jnp.float32), pad], axis=0).T
            j = lax.broadcasted_iota(jnp.int32, (1, COLS), 1)
            number = (z * NY + y) * (2 * NX) + x * 2
            start = jnp.where(j < SLOT, (number + c) * WID, (number + 1 - c) * WID - SLOT)
            inside = jnp.where(j < SLOT, j, j - SLOT) < WID
            cols[...] = jnp.where(inside, start + j, 1 << 28).astype(jnp.float32)

        def one(r, carry):
            column = jnp.sum(jnp.where(lanes == r, turned[0], 0.0), axis=1, keepdims=True)
            lim_col[pl.ds(pl.multiple_of(r * 128, 128), 128), :] = jnp.broadcast_to(column, (128, 128))
            return carry

        lax.fori_loop(4 * k, 4 * k + 4, one, 0)

    def places():
        for k in range(3):
            column = jnp.sum(jnp.where(lanes == 3 * z + k, turned[1], 0.0), axis=1, keepdims=True)
            pos_col[k * 128:(k + 1) * 128, :] = jnp.broadcast_to(column, (128, 128))
        slab[...] = jnp.zeros_like(slab)

    def settle(which, k):
        def one(r, carry):
            rows = pl.ds(pl.multiple_of(r * 128, 128), 128)
            weight[rows, which * SLOT:which * SLOT + WID] = stage[which, rows, :]
            return carry

        lax.fori_loop(14 * k, 14 * k + 14, one, 0)

    def mask_z(dz):
        return pltpu.make_async_remote_copy(
            src_ref=masks.at[0, 0], dst_ref=masks.at[8 - dz, 0], send_sem=mz_sem.at[0, dz],
            recv_sem=mz_sem.at[1, 8 - dz], device_id=device(z=dz), device_id_type=MESH)

    def mask_y(dy):
        return pltpu.make_async_remote_copy(
            src_ref=masks.at[:, 0], dst_ref=masks.at[:, 4 - dy], send_sem=my_sem.at[0, dy],
            recv_sem=my_sem.at[1, 4 - dy], device_id=device(y=dy), device_id_type=MESH)

    def mask_arrived_z(dz):
        return pltpu.make_async_remote_copy(
            src_ref=masks.at[0, 0], dst_ref=masks.at[dz, 0], send_sem=mz_sem.at[0, dz],
            recv_sem=mz_sem.at[1, dz], device_id=device(z=dz), device_id_type=MESH)

    def mask_arrived_y(dy):
        return pltpu.make_async_remote_copy(
            src_ref=masks.at[:, 0], dst_ref=masks.at[:, dy], send_sem=my_sem.at[0, dy],
            recv_sem=my_sem.at[1, dy], device_id=device(y=dy), device_id_type=MESH)

    def prep(name, k):
        if name == "limits":
            limits(k)
        elif name == "places":
            places()
        elif name == "own":
            if k == 0:
                own_w.wait()
            settle(0, k)
        elif name == "other":
            if k == 0:
                give_w.wait_recv()
            settle(1, k)
        elif k == 0:
            for dz in range(1, NZ):
                mask_z(dz).start()
        else:
            for dz in range(1, NZ):
                mask_arrived_z(dz).wait_recv()
            for dy in range(1, NY):
                mask_y(dy).start()

    def window(dz):
        rows = held.at[dz]

        def multiply(n, carry):
            at = pl.ds(pl.multiple_of(n * TILE, TILE), TILE)
            logits[:, at] = jnp.dot(rows[...].reshape(ROWS, D), weight[:, at],
                                    preferred_element_type=jnp.float32)
            return carry

        lax.fori_loop(0, COLS // TILE, multiply, 0)
        source_z = lax.rem(z + dz, NZ)

        def group(dy, carry):
            source_y = lax.rem(y + dy, NY)
            first_row = (source_z * NY + source_y) * TOK + c * HALF
            limit = lim_col[pl.ds(pl.multiple_of(first_row, RB), HALF), :]
            peak = jnp.full((HALF, 128), NEG, jnp.float32)
            kept = []
            for j in range(COLS // 128):
                part = logits[pl.ds(pl.multiple_of(dy * HALF, RB), HALF), j * 128:(j + 1) * 128]
                part = jnp.where(cols[:, j * 128:(j + 1) * 128] < limit, part, NEG)
                kept.append(part)
                peak = jnp.maximum(peak, part)
            peak = jnp.max(peak, axis=1, keepdims=True)
            total = jnp.zeros((HALF, 128), jnp.float32)
            moment = jnp.zeros((HALF, 128), jnp.float32)
            for part in kept:
                shifted = part - peak
                e = jnp.exp(shifted)
                total = total + e
                moment = moment + e * shifted
            total = jnp.sum(total, axis=1, keepdims=True)
            moment = jnp.sum(moment, axis=1, keepdims=True)
            lane = lanes[:HALF]
            slab[pl.ds(pl.multiple_of(source_y * 64, 64), HALF), :] = jnp.where(
                lane == 0, peak, jnp.where(lane == 1, total, moment))
            return carry

        lax.fori_loop(0, NY, group, 0)
        across = slab[...].T
        for k in range(3):
            stat[dz, k] = across[k:k + 1]
        if dz:
            stat_copy(dz).start()

    def stat_copy(dz):
        return pltpu.make_async_remote_copy(
            src_ref=stat.at[dz], dst_ref=from_z.at[8 - dz], send_sem=rz_sem.at[0, dz],
            recv_sem=rz_sem.at[1, 8 - dz], device_id=device(z=dz), device_id_type=MESH)

    masks[0, 0] = jnp.zeros((1, 128), jnp.float32)
    masks[0, 0, :, 0:TOK] = mask_ref[...].astype(jnp.float32)
    first_send = True
    for step in STEPS:
        if step[0] == "send":
            _, axis, m, q = step
            started[q] = transfer(q, axis, m)
            started[q].start()
        else:
            if first_send:
                give_w.start()
                first_send = False
            if step[0] == "wait":
                started[step[1]].wait_recv()
            elif step[0] == "prep":
                prep(*step[1])
            else:
                window(step[1])

    for dz in range(1, NZ):
        pltpu.make_async_remote_copy(
            src_ref=stat.at[dz], dst_ref=from_z.at[dz], send_sem=rz_sem.at[0, dz],
            recv_sem=rz_sem.at[1, dz], device_id=device(z=dz), device_id_type=MESH).wait_recv()
    parts = [tuple(stat[0, k] for k in range(3))]
    parts += [tuple(from_z[dz, k] for k in range(3)) for dz in range(1, NZ)]
    merged = merge(parts)
    for k in range(3):
        plane[k] = merged[k]

    spots = [(dy, dx) for dy in range(NY) for dx in range(NX) if dy or dx]

    def plane_copy(dy, dx, arrive):
        back = (NY - dy) % NY * NX + (NX - dx) % NX
        slot = dy * NX + dx if arrive else back
        return pltpu.make_async_remote_copy(
            src_ref=plane, dst_ref=from_plane.at[slot], send_sem=rp_sem.at[0, dy * NX + dx],
            recv_sem=rp_sem.at[1, slot], device_id=device(y=dy, x=dx), device_id_type=MESH)

    for dy, dx in spots:
        plane_copy(dy, dx, False).start()
    for dy in range(1, NY):
        mask_arrived_y(dy).wait_recv()
    for dy, dx in spots:
        plane_copy(dy, dx, True).wait_recv()
    parts = [merged] + [tuple(from_plane[dy * NX + dx, k] for k in range(3)) for dy, dx in spots]
    peak, total, moment = merge(parts)
    entropy = jnp.log(total) - moment / total

    masked = jnp.zeros((1, 128), jnp.float32)
    found = []
    for k in range(2):
        owner = jnp.where(c == 0, 2 * z + k, 31 - 2 * z - k)
        column = jnp.broadcast_to(entropy[:, k * 128:(k + 1) * 128], (128, 128)).T
        spot = (owner * TOK).astype(jnp.float32) + lanes[:HALF].astype(jnp.float32)
        here_e = jnp.zeros((HALF, 128), jnp.float32)
        for h in range(2):
            source = pl.multiple_of((2 * k + h) * TOK + c * HALF, RB)
            here_e = here_e + jnp.where(pos_col[pl.ds(source, HALF), :] == spot,
                                        column[h * 64:h * 64 + HALF], 0.0)
        here_e = jnp.sum(here_e, axis=0, keepdims=True)
        found.append(here_e)
        dz = lax.rem(owner // NY - z + NZ, NZ)
        dy = lax.rem(lax.rem(owner, NY) - y + NY, NY)
        masked = masked + here_e * masks[dz, dy]
    masked = jnp.sum(masked, axis=1, keepdims=True)
    lane = lanes[:1]
    for k in range(2):
        ents[0, 0, k] = jnp.where(lane < TOK, found[k], masked if k == 0 else 0.0)

    others = [(dz, other) for dz in range(NZ) for other in range(2) if dz or other]

    def ent_copy(dz, other, arrive):
        slot = dz if arrive else (NZ - dz) % NZ
        target = device(z=dz, c=1) if other else device(z=dz)
        return pltpu.make_async_remote_copy(
            src_ref=ents.at[0, 0], dst_ref=ents.at[slot, other], send_sem=re_sem.at[0, dz, other],
            recv_sem=re_sem.at[1, slot, other], device_id=target, device_id_type=MESH)

    for dz, other in others:
        ent_copy(dz, other, False).start()

    started_count = jnp.sum(jnp.sum(masks[...].reshape(NZ * NY, 128), axis=0, keepdims=True), axis=1, keepdims=True)
    for k in range(len(TRANSFERS)):
        started[TRANSFERS[k]].wait_send()
    swap.wait_send()
    give_w.wait_send()
    for dz in range(1, NZ):
        mask_z(dz).wait_send()
        stat_copy(dz).wait_send()
    for dy in range(1, NY):
        mask_y(dy).wait_send()
    for dy, dx in spots:
        plane_copy(dy, dx, False).wait_send()

    for dz, other in others:
        ent_copy(dz, other, True).wait_recv()
    total_masked = jnp.zeros((1, 1), jnp.float32)
    for dz in range(NZ):
        for other in range(2):
            total_masked = total_masked + ents[dz, other, 0][:, TOK:TOK + 1]
    mean = total_masked / jnp.maximum(started_count, 1.0)
    mean_ref[...] = jnp.broadcast_to(mean, (1, 128))
    mine_s = z * NY + y
    index = jnp.where(z < NZ // 2, mine_s, 31 - mine_s)
    dz = lax.rem(index // 2 - z + NZ, NZ)
    other = jnp.where(z < NZ // 2, c, 1 - c)
    ent_ref[...] = ents[dz, other, lax.rem(index, 2)]
    for dz, other in others:
        ent_copy(dz, other, False).wait_send()


def local(hidden, lm_head, positions, vocab_limits, loss_mask):
    f32, bf16 = jnp.float32, jnp.bfloat16
    dma = pltpu.SemaphoreType.DMA
    any_space = pl.BlockSpec(memory_space=pl.ANY)
    vmem = pl.BlockSpec(memory_space=pltpu.VMEM)
    count = len(TRANSFERS)
    ent, mean = pl.pallas_call(
        kernel,
        out_shape=(jax.ShapeDtypeStruct((1, 128), f32), jax.ShapeDtypeStruct((1, 128), f32)),
        in_specs=[any_space, any_space, vmem, vmem, vmem],
        out_specs=(vmem, vmem),
        scratch_shapes=[
            pltpu.VMEM((NZ, NY, COLORS, RB, D), bf16),
            pltpu.VMEM((D, COLS), bf16),
            pltpu.VMEM((2, D, WID), bf16),
            pltpu.VMEM((TOK, FEAT // 2), bf16),
            pltpu.VMEM((HALF, FEAT // 2), bf16),
            pltpu.VMEM((ROWS, COLS), f32),
            pltpu.VMEM((2, 128, 128), f32),
            pltpu.VMEM((NZ * NY * TOK, 128), f32),
            pltpu.VMEM((3 * 128, 128), f32),
            pltpu.VMEM((1, COLS), f32),
            pltpu.VMEM((256, 128), f32),
            pltpu.VMEM((NZ, 3, 1, 256), f32),
            pltpu.VMEM((NZ, 3, 1, 256), f32),
            pltpu.VMEM((3, 1, 256), f32),
            pltpu.VMEM((NY * NX, 3, 1, 256), f32),
            pltpu.VMEM((NZ, 2, 2, 1, 128), f32),
            pltpu.VMEM((NZ, NY, 1, 128), f32),
            dma((count,)), dma((count,)), dma((2,)), dma((2,)),
            dma((2, NZ)), dma((2, NY)), dma((2, NZ)), dma((2, NY * NX)), dma((2, NZ, 2)), dma((2,)),
        ],
        compiler_params=pltpu.CompilerParams(
            collective_id=0, has_side_effects=True, vmem_limit_bytes=62 * 2**20),
    )(hidden, lm_head, positions.reshape(24, 128), vocab_limits.reshape(24, 128), loss_mask.reshape(1, TOK))
    return ent[0, :TOK], mean[0, 0]


def solution(mesh):
    torus = Mesh(mesh.devices.reshape(NZ, NY, NX, 2), AXES)
    in_specs = (P(("z", "y"), ("x", "c")), P(None, AXES), P(), P(), P(("z", "y")))
    return jax.shard_map(local, mesh=torus, in_specs=in_specs, out_specs=(P(("z", "y")), P()), check_vma=False)
```

```python
import heapq

import jax
import jax.numpy as jnp
from jax import lax
from jax.experimental import pallas as pl
from jax.experimental.pallas import tpu as pltpu
from jax.sharding import Mesh
from jax.sharding import PartitionSpec as P

NZ, NY, NX = 8, 4, 4
SIZE = {"z": NZ, "y": NY, "x": NX}
AXES = ("z", "y", "x", "c")
MESH = pl.DeviceIdType.MESH
HALF, RB, COLORS = 48, 16, 3
TOK = 96
D, FEAT = 3584, 896
WID, PAD = 594, 608
GROUP = 64
LANES = NY * GROUP
NEG = -1e30
ORDER = (1, 7, 2, 6, 3, 5, 4, 0)
DEADLINE = (17.7, 10.3, 11.8, 14.5, 16.9, 16.7, 12.6, 10.1)
UNIT, HOP, BACKLOG = 0.615, 1.75, 1.5
WINDOW = 2.6


def onward(n, d, far):
    if d == 0:
        return [1, -1]
    if d < n // 2:
        return [-1] if d + 1 < n // 2 or far == -1 else []
    if d > n // 2:
        return [1] if d - 1 > n // 2 or far == 1 else []
    return []


def parity(k):
    return 1 if k % 2 == 0 else -1


def sends_of(p):
    color, axis, rest = p[0], p[1], p[2:]
    out = []
    if color == "A" and axis == "y":
        (dy,) = rest
        out += [("y", m, 1, ("A", "y", (dy - m) % 4)) for m in onward(4, dy, 1)]
        out += [("x", m, 1, ("A", "x", dy, -m % 4)) for m in (1, -1)]
    elif color == "A" and axis == "x":
        dy, dx = rest
        out += [("x", m, 1, ("A", "x", dy, (dx - m) % 4)) for m in onward(4, dx, parity(dy))]
    elif color == "A":
        dz, dy = rest
        out += [("z", m, 4, ("A", "z", (dz - m) % 8, dy)) for m in onward(8, dz, parity(dy))]
    elif axis == "z":
        (dz,) = rest
        far = 1 if color == "B" else -1
        out += [("z", m, 1, (color, "z", (dz - m) % 8)) for m in onward(8, dz, far)]
        second = "y" if color == "B" else "x"
        out += [(second, m, 1, (color, second, dz, -m % 4)) for m in (1, -1)]
    else:
        dz, d = rest
        last = (color, axis) in (("B", "x"), ("C", "y"))
        size = 4 if last else 1
        out += [(axis, m, size, (color, axis, dz, (d - m) % 4)) for m in onward(4, d, parity(dz))]
    return out


def launch_of(p):
    color, axis = p[0], p[1]
    if color == "A" and axis != "z":
        return ("A", "z", 0, p[2])
    if color == "B" and axis != "x":
        return ("B", "x", p[2], 0)
    if color == "C" and axis != "y":
        return ("C", "y", p[2], 0)
    return None


def parts_of(launch):
    color, _, a, b = launch
    if color == "A":
        return [("A", "y", b)] + [("A", "x", b, k) for k in (1, 2, 3)]
    if color == "B":
        return [("B", "z", a)] + [("B", "y", a, k) for k in (1, 2, 3)]
    return [("C", "z", a)] + [("C", "x", a, k) for k in (1, 2, 3)]


def window_of(p):
    return 0 if p[0] == "A" and p[1] != "z" else p[2]


def pieces_of_window(dz):
    need = [("B", "x", dz, k) for k in range(4)] + [("C", "y", dz, k) for k in range(4)]
    return need + [("A", "z", dz, k) for k in range(4)]


def plan(preps):
    due = {}

    def latest(p):
        if p not in due:
            dz = window_of(p)
            k = DEADLINE[dz]
            ahead = sends_of(p)
            launch = launch_of(p)
            if launch:
                ahead = ahead + sends_of(launch)
            for _, _, size, q in ahead:
                k = min(k, latest(q) - HOP - size * UNIT - 0.3)
            due[p] = k
        return due[p]

    free = {(a, m): 0.0 for a in "xyz" for m in (1, -1)}
    waiting = {k: [] for k in free}
    have, steps, flying = set(), [], []
    count = 0
    now = 0.0

    def offer(sends):
        nonlocal count
        for axis, m, size, q in sends:
            heapq.heappush(waiting[axis, m], (latest(q) - size * UNIT, count, size, q))
            count += 1

    def pump():
        nonlocal count
        for link in free:
            while waiting[link] and free[link] - now < BACKLOG:
                _, _, size, q = heapq.heappop(waiting[link])
                free[link] = max(free[link], now) + size * UNIT
                heapq.heappush(flying, (free[link] + HOP, count, q))
                count += 1
                steps.append(("send", link[0], link[1], q))

    def take(p):
        have.add(p)
        offer(sends_of(p))
        launch = launch_of(p)
        if launch and launch not in have and all(q in have for q in parts_of(launch)):
            have.add(launch)
            offer(sends_of(launch))

    def blocked():
        return any(p[0][0] == "other" for p in preps)

    for p in (("A", "y", 0), ("B", "z", 0), ("C", "z", 0)):
        take(p)
    pump()
    left = list(ORDER)
    preps = list(preps)
    while flying or left or preps:
        if flying and flying[0][0] <= now:
            _, _, q = heapq.heappop(flying)
            steps.append(("wait", q))
            take(q)
            pump()
            now += 0.03
            continue
        if preps and now >= preps[0][1]:
            name, _, cost = preps.pop(0)
            steps.append(("prep", name))
            now += cost
            pump()
            continue
        ready = [] if blocked() else [w for w in left if all(q in have for q in pieces_of_window(w))]
        if len(left) > 1:
            ready = [w for w in ready if w]
        if ready:
            steps.append(("window", ready[0]))
            left.remove(ready[0])
            now += WINDOW
            pump()
            continue
        nxt = [flying[0][0]] if flying else []
        if preps:
            nxt.append(preps[0][1])
        now = max(now, min(nxt))
    return steps, now


PREPS = (
    [(("limits", 0), 0.2, 0.3), (("places", 0), 0.8, 0.4)]
    + [(("own", k), 3.0, 0.3) for k in range(2)]
    + [(("other", k), 11.0, 0.3) for k in range(2)]
    + [(("mask", 0), 16.0, 0.1), (("mask", 1), 32.0, 0.1)]
)
STEPS, _ = plan(PREPS)
TRANSFERS = [s[3] for s in STEPS if s[0] == "send"]
NUMBER = {q: k for k, q in enumerate(TRANSFERS)}


def merge(parts):
    peak = parts[0][0]
    for p in parts[1:]:
        peak = jnp.maximum(peak, p[0])
    total = jnp.zeros_like(peak)
    moment = jnp.zeros_like(peak)
    for m, t, mo in parts:
        shift = m - peak
        ratio = jnp.exp(shift)
        total = total + ratio * t
        moment = moment + ratio * (mo + t * shift)
    return peak, total, moment


def kernel(hid_ref, lm_ref, pos_ref, lim_ref, mask_ref, ent_ref, mean_ref,
           held, weight, stage, hstage, pstage, logits, small, mask_in, lim_row, pos_col,
           stat, from_z, plane, from_plane, ents, masks,
           send_sem, recv_sem, hx_sem, w_sem, mz_sem, my_sem, rz_sem, rp_sem, re_sem, copy_sem):
    z, y, x, c = (lax.axis_index(a) for a in AXES)
    here = {"z": z, "y": y, "x": x, "c": c}

    def device(**moved):
        return tuple(lax.rem(here[a] + moved[a], SIZE[a]) if a in moved and a != "c" else
                     (1 - c if a in moved else here[a]) for a in AXES)

    own_w = pltpu.make_async_copy(lm_ref, stage.at[0], copy_sem.at[0])
    own_h = pltpu.make_async_copy(hid_ref, hstage, copy_sem.at[1])
    own_h.start()
    own_w.start()
    given = [pltpu.make_async_copy(lim_ref, small.at[0], copy_sem.at[2]),
             pltpu.make_async_copy(pos_ref, small.at[1], copy_sem.at[3]),
             pltpu.make_async_copy(mask_ref, mask_in, copy_sem.at[4])]
    for copy in given:
        copy.start()

    barrier = pltpu.get_barrier_semaphore()
    near = [device(**{a: d}) for a in "zyx" for d in (1, SIZE[a] - 1)] + [device(c=1)]
    for who in near:
        pl.semaphore_signal(barrier, inc=1, device_id=who, device_id_type=MESH)
    with jax.named_scope("T_barrier"):
        pl.semaphore_wait(barrier, len(near))

    with jax.named_scope("T_ownh"):
        own_h.wait()
    swap = pltpu.make_async_remote_copy(
        src_ref=hstage.at[pl.ds(pl.multiple_of((1 - c) * HALF, RB), HALF), :], dst_ref=pstage,
        send_sem=hx_sem.at[0], recv_sem=hx_sem.at[1], device_id=device(c=1), device_id_type=MESH)
    swap.start()
    give_w = pltpu.make_async_remote_copy(
        src_ref=lm_ref, dst_ref=stage.at[1],
        send_sem=w_sem.at[0], recv_sem=w_sem.at[1], device_id=device(c=1), device_id_type=MESH)

    def feature(dx):
        return pl.ds(pl.multiple_of(lax.rem(x + dx, NX) * FEAT, 128), FEAT)

    mine = hstage[pl.ds(pl.multiple_of(c * HALF, RB), HALF), :].astype(jnp.float32)
    with jax.named_scope("T_swap"):
        swap.wait_recv()
    theirs = pstage[...].astype(jnp.float32)
    first = c == 0
    left = jnp.where(first, mine, theirs)
    right = jnp.where(first, theirs, mine)
    both = jnp.concatenate([left, right], axis=1).astype(jnp.bfloat16)
    for k in range(COLORS):
        held[0, 0, k * RB:(k + 1) * RB, feature(0)] = both[k * RB:(k + 1) * RB]

    def block(k):
        return pl.ds(k * RB, RB)

    def place(p):
        color, axis = p[0], p[1]
        if color == "A":
            if axis == "z":
                return held.at[p[2], p[3], block(0)]
            return held.at[0, p[2], block(0), feature(0 if axis == "y" else p[3])]
        if axis == "z":
            return held.at[p[2], 0, block(1 if color == "B" else 2), feature(0)]
        if color == "B":
            if axis == "y":
                return held.at[p[2], p[3], block(1), feature(0)]
            return held.at[p[2], :, block(1), feature(p[3])]
        if axis == "x":
            return held.at[p[2], 0, block(2), feature(p[3])]
        return held.at[p[2], p[3], block(2)]

    def transfer(q, axis, m):
        k = NUMBER[q]
        n = SIZE[axis]
        if axis == "x":
            source = q[:-1] + ((q[-1] + m) % n,)
        else:
            at = {("A", "y"): 2, ("A", "z"): 2, ("B", "z"): 2, ("C", "z"): 2}.get(q[:2], 3)
            source = q[:at] + ((q[at] + m) % n,) + q[at + 1:]
        if (q[0], axis) in (("A", "x"), ("B", "y"), ("C", "x")) and source[3] == 0:
            source = (q[0], "y" if q[0] == "A" else "z", q[2])
        dst = place(q)
        if axis == "x":
            src = dst_at = None
            column = feature(q[-1] + m + NX)
            if q[0] == "A":
                src = dst_at = held.at[0, q[2], block(0), column]
            elif q[0] == "B":
                src = dst_at = held.at[q[2], :, block(1), column]
            else:
                src = dst_at = held.at[q[2], 0, block(2), column]
            dst = dst_at
        else:
            src = place(source)
        return pltpu.make_async_remote_copy(
            src_ref=src, dst_ref=dst, send_sem=send_sem.at[k], recv_sem=recv_sem.at[k],
            device_id=device(**{axis: m % n}), device_id_type=MESH)

    started = {}
    lanes = lax.broadcasted_iota(jnp.int32, (128, 128), 1)

    def limits():
        for copy in given:
            copy.wait()
        masks[0, 0] = jnp.zeros((1, 128), jnp.float32)
        masks[0, 0, :, 0:TOK] = mask_in[...].astype(jnp.float32)
        table = jnp.concatenate([small[0, pl.ds(j, NZ, stride=3), :] for j in range(3)], axis=1)
        row = lax.broadcasted_iota(jnp.int32, (3 * 128, LANES), 0)
        column = lax.broadcasted_iota(jnp.int32, (3 * 128, LANES), 1)
        dy, i = column // GROUP, column % GROUP
        want = lax.rem(y + dy, NY) * TOK + c * HALF + i
        pick = jnp.where((row == want) & (i < HALF), 1.0, 0.0).astype(jnp.bfloat16)
        found = jnp.zeros((NZ, LANES), jnp.float32)
        for shift in (14, 7, 0):
            digit = lax.bitwise_and(lax.shift_right_logical(table, shift), 127)
            digit = digit.astype(jnp.float32).astype(jnp.bfloat16)
            found = found * 128.0 + jnp.dot(digit, pick, preferred_element_type=jnp.float32)
        lim_row[...] = found.astype(jnp.int32)

    def places():
        pad = jnp.zeros((128 - 24, 128), jnp.float32)
        turned = jnp.concatenate([small[1].astype(jnp.float32), pad], axis=0).T
        for k in range(3):
            column = jnp.sum(jnp.where(lanes == 3 * z + k, turned, 0.0), axis=1, keepdims=True)
            pos_col[k * 128:(k + 1) * 128, :] = jnp.broadcast_to(column, (128, 128))

    def settle(which, k):
        def one(r, carry):
            at = pl.ds(pl.multiple_of(r * 256, 128), 256)
            weight[which, 0:WID, at] = stage[which, :, at]
            return carry

        lax.fori_loop(7 * k, 7 * k + 7, one, 0)

    def mask_z(dz):
        return pltpu.make_async_remote_copy(
            src_ref=masks.at[0, 0], dst_ref=masks.at[8 - dz, 0], send_sem=mz_sem.at[0, dz],
            recv_sem=mz_sem.at[1, 8 - dz], device_id=device(z=dz), device_id_type=MESH)

    def mask_y(dy):
        return pltpu.make_async_remote_copy(
            src_ref=masks.at[:, 0], dst_ref=masks.at[:, 4 - dy], send_sem=my_sem.at[0, dy],
            recv_sem=my_sem.at[1, 4 - dy], device_id=device(y=dy), device_id_type=MESH)

    def mask_arrived_z(dz):
        return pltpu.make_async_remote_copy(
            src_ref=masks.at[0, 0], dst_ref=masks.at[dz, 0], send_sem=mz_sem.at[0, dz],
            recv_sem=mz_sem.at[1, dz], device_id=device(z=dz), device_id_type=MESH)

    def mask_arrived_y(dy):
        return pltpu.make_async_remote_copy(
            src_ref=masks.at[:, 0], dst_ref=masks.at[:, dy], send_sem=my_sem.at[0, dy],
            recv_sem=my_sem.at[1, dy], device_id=device(y=dy), device_id_type=MESH)

    def prep(name, k):
        if name == "limits":
            limits()
        elif name == "places":
            places()
        elif name == "own":
            if k == 0:
                own_w.wait()
            settle(0, k)
        elif name == "other":
            if k == 0:
                give_w.wait_recv()
            settle(1, k)
        elif k == 0:
            for dz in range(1, NZ):
                mask_z(dz).start()
        else:
            for dz in range(1, NZ):
                mask_arrived_z(dz).wait_recv()
            for dy in range(1, NY):
                mask_y(dy).start()

    number = (z * NY + y) * (2 * NX) + x * 2
    starts = ((number + c) * WID, (number + 1 - c) * WID)
    depth = lax.broadcasted_iota(jnp.int32, (PAD, LANES), 0)

    def multiply(dz, slot):
        for k in range(2):
            logits[slot, k] = lax.dot_general(
                weight[k], held[dz].reshape(LANES, D), (((1,), (1,)), ((), ())),
                preferred_element_type=jnp.float32)

    def reduce_rows(dz, slot):
        limit = lim_row[pl.ds(lax.rem(z + dz, NZ), 1), :]
        peak = jnp.full((1, LANES), NEG, jnp.float32)
        for k in range(2):
            bound = jnp.minimum(limit - starts[k], WID)
            logits[slot, k] = jnp.where(depth < bound, logits[slot, k], NEG)
            peak = jnp.maximum(peak, jnp.max(logits[slot, k], axis=0, keepdims=True))
        total = jnp.zeros((1, LANES), jnp.float32)
        moment = jnp.zeros((1, LANES), jnp.float32)
        for k in range(2):
            shifted = logits[slot, k] - peak
            e = jnp.exp(shifted)
            total = total + jnp.sum(e, axis=0, keepdims=True)
            moment = moment + jnp.sum(e * shifted, axis=0, keepdims=True)
        rows = jnp.concatenate([peak, total, moment, jnp.zeros((5, LANES), jnp.float32)], axis=0)
        rows = pltpu.roll(rows, y * GROUP, 1)
        for k in range(3):
            stat[dz, k] = rows[k:k + 1]
        if dz:
            stat_copy(dz).start()

    def stat_copy(dz):
        return pltpu.make_async_remote_copy(
            src_ref=stat.at[dz], dst_ref=from_z.at[8 - dz], send_sem=rz_sem.at[0, dz],
            recv_sem=rz_sem.at[1, 8 - dz], device_id=device(z=dz), device_id_type=MESH)

    done = []

    def window(dz):
        if done:
            reduce_rows(done[-1], len(done) % 2)
        if dz is None:
            return
        done.append(dz)
        multiply(dz, len(done) % 2)

    first_send = True
    for step in STEPS:
        if step[0] == "send":
            _, axis, m, q = step
            started[q] = transfer(q, axis, m)
            started[q].start()
        else:
            if first_send:
                give_w.start()
                first_send = False
            if step[0] == "wait":
                started[step[1]].wait_recv()
            elif step[0] == "prep":
                prep(*step[1])
            else:
                window(step[1])
    with jax.named_scope("T_last"):
        window(None)

    with jax.named_scope("T_zround"):
        for dz in range(1, NZ):
            pltpu.make_async_remote_copy(
                src_ref=stat.at[dz], dst_ref=from_z.at[dz], send_sem=rz_sem.at[0, dz],
                recv_sem=rz_sem.at[1, dz], device_id=device(z=dz), device_id_type=MESH).wait_recv()
    parts = [tuple(stat[0, k] for k in range(3))]
    parts += [tuple(from_z[dz, k] for k in range(3)) for dz in range(1, NZ)]
    merged = merge(parts)
    for k in range(3):
        plane[k] = merged[k]

    spots = [(dy, dx) for dy in range(NY) for dx in range(NX) if dy or dx]

    def plane_copy(dy, dx, arrive):
        back = (NY - dy) % NY * NX + (NX - dx) % NX
        slot = dy * NX + dx if arrive else back
        return pltpu.make_async_remote_copy(
            src_ref=plane, dst_ref=from_plane.at[slot], send_sem=rp_sem.at[0, dy * NX + dx],
            recv_sem=rp_sem.at[1, slot], device_id=device(y=dy, x=dx), device_id_type=MESH)

    for dy, dx in spots:
        plane_copy(dy, dx, False).start()
    for dy in range(1, NY):
        mask_arrived_y(dy).wait_recv()
    with jax.named_scope("T_planeround"):
        for dy, dx in spots:
            plane_copy(dy, dx, True).wait_recv()
    parts = [merged] + [tuple(from_plane[dy * NX + dx, k] for k in range(3)) for dy, dx in spots]
    peak, total, moment = merge(parts)
    entropy = jnp.log(total) - moment / total

    masked = jnp.zeros((1, 128), jnp.float32)
    found = []
    for k in range(2):
        owner = jnp.where(c == 0, 2 * z + k, 31 - 2 * z - k)
        column = jnp.broadcast_to(entropy[:, k * 128:(k + 1) * 128], (128, 128)).T
        spot = (owner * TOK).astype(jnp.float32) + lanes[:HALF].astype(jnp.float32)
        here_e = jnp.zeros((HALF, 128), jnp.float32)
        for h in range(2):
            source = pl.multiple_of((2 * k + h) * TOK + c * HALF, RB)
            here_e = here_e + jnp.where(pos_col[pl.ds(source, HALF), :] == spot,
                                        column[h * 64:h * 64 + HALF], 0.0)
        here_e = jnp.sum(here_e, axis=0, keepdims=True)
        found.append(here_e)
        dz = lax.rem(owner // NY - z + NZ, NZ)
        dy = lax.rem(lax.rem(owner, NY) - y + NY, NY)
        masked = masked + here_e * masks[dz, dy]
    masked = jnp.sum(masked, axis=1, keepdims=True)
    lane = lanes[:1]
    for k in range(2):
        ents[0, 0, k] = jnp.where(lane < TOK, found[k], masked if k == 0 else 0.0)

    others = [(dz, other) for dz in range(NZ) for other in range(2) if dz or other]

    def ent_copy(dz, other, arrive):
        slot = dz if arrive else (NZ - dz) % NZ
        target = device(z=dz, c=1) if other else device(z=dz)
        return pltpu.make_async_remote_copy(
            src_ref=ents.at[0, 0], dst_ref=ents.at[slot, other], send_sem=re_sem.at[0, dz, other],
            recv_sem=re_sem.at[1, slot, other], device_id=target, device_id_type=MESH)

    for dz, other in others:
        ent_copy(dz, other, False).start()

    started_count = jnp.sum(jnp.sum(masks[...].reshape(NZ * NY, 128), axis=0, keepdims=True), axis=1, keepdims=True)
    for k in range(len(TRANSFERS)):
        started[TRANSFERS[k]].wait_send()
    swap.wait_send()
    give_w.wait_send()
    for dz in range(1, NZ):
        mask_z(dz).wait_send()
        stat_copy(dz).wait_send()
    for dy in range(1, NY):
        mask_y(dy).wait_send()
    for dy, dx in spots:
        plane_copy(dy, dx, False).wait_send()

    with jax.named_scope("T_entround"):
        for dz, other in others:
            ent_copy(dz, other, True).wait_recv()
    total_masked = jnp.sum(ents[:, :, 0].reshape(2 * NZ, 128), axis=0, keepdims=True)
    total_masked = jnp.sum(jnp.where(lane == TOK, total_masked, 0.0), axis=1, keepdims=True)
    mean = total_masked / jnp.maximum(started_count, 1.0)
    mean_ref[...] = jnp.broadcast_to(mean, (1, 128))
    mine_s = z * NY + y
    index = jnp.where(z < NZ // 2, mine_s, 31 - mine_s)
    dz = lax.rem(index // 2 - z + NZ, NZ)
    other = jnp.where(z < NZ // 2, c, 1 - c)
    ent_ref[...] = ents[dz, other, lax.rem(index, 2)][:, 0:TOK]
    for dz, other in others:
        ent_copy(dz, other, False).wait_send()


def local(hidden, lm_head, positions, vocab_limits, loss_mask):
    f32, bf16 = jnp.float32, jnp.bfloat16
    dma = pltpu.SemaphoreType.DMA
    any_space = pl.BlockSpec(memory_space=pl.ANY)
    vmem = pl.BlockSpec(memory_space=pltpu.VMEM)
    count = len(TRANSFERS)
    ent, mean = pl.pallas_call(
        kernel,
        out_shape=(jax.ShapeDtypeStruct((1, TOK), f32), jax.ShapeDtypeStruct((1, 128), f32)),
        in_specs=[any_space] * 5,
        out_specs=(vmem, vmem),
        scratch_shapes=[
            pltpu.VMEM((NZ, NY, GROUP, D), bf16),
            pltpu.VMEM((2, PAD, D), bf16),
            pltpu.VMEM((2, WID, D), bf16),
            pltpu.VMEM((TOK, FEAT // 2), bf16),
            pltpu.VMEM((HALF, FEAT // 2), bf16),
            pltpu.VMEM((2, 2, PAD, LANES), f32),
            pltpu.VMEM((2, 24, 128), jnp.int32),
            pltpu.VMEM((1, TOK), jnp.int32),
            pltpu.VMEM((NZ, LANES), jnp.int32),
            pltpu.VMEM((3 * 128, 128), f32),
            pltpu.VMEM((NZ, 3, 1, 256), f32),
            pltpu.VMEM((NZ, 3, 1, 256), f32),
            pltpu.VMEM((3, 1, 256), f32),
            pltpu.VMEM((NY * NX, 3, 1, 256), f32),
            pltpu.VMEM((NZ, 2, 2, 1, 128), f32),
            pltpu.VMEM((NZ, NY, 1, 128), f32),
            dma((count,)), dma((count,)), dma((2,)), dma((2,)),
            dma((2, NZ)), dma((2, NY)), dma((2, NZ)), dma((2, NY * NX)), dma((2, NZ, 2)), dma((5,)),
        ],
        compiler_params=pltpu.CompilerParams(
            collective_id=0, has_side_effects=True, vmem_limit_bytes=62 * 2**20),
    )(hidden, lm_head.T, positions.reshape(24, 128), vocab_limits.reshape(24, 128), loss_mask.reshape(1, TOK))
    return ent.reshape(TOK), mean[0, 0]


def solution(mesh):
    torus = Mesh(mesh.devices.reshape(NZ, NY, NX, 2), AXES)
    in_specs = (P(("z", "y"), ("x", "c")), P(None, AXES), P(), P(), P(("z", "y")))
    return jax.shard_map(local, mesh=torus, in_specs=in_specs, out_specs=(P(("z", "y")), P()), check_vma=False)
```

```python
import heapq

import jax
import jax.numpy as jnp
from jax import lax
from jax.experimental import pallas as pl
from jax.experimental.pallas import tpu as pltpu
from jax.sharding import Mesh
from jax.sharding import PartitionSpec as P

NZ, NY, NX = 8, 4, 4
SIZE = {"z": NZ, "y": NY, "x": NX}
AXES = ("z", "y", "x", "c")
MESH = pl.DeviceIdType.MESH
HALF, RB, COLORS = 48, 16, 3
TOK = 96
D, FEAT = 3584, 896
WID, PAD = 594, 608
CHUNK, LANES = 64, 256
WINDOWS = NZ * COLORS * CHUNK // LANES
NEG = -1e30
DEADLINE = (
    (18.1, 16.1, 16.7),
    (19.9, 17.9, 18.5),
    (23.9, 21.9, 22.5),
    (24.8, 22.8, 23.4),
    (26.9, 24.9, 25.5),
    (24.1, 22.1, 22.7),
    (24.2, 22.2, 22.8),
    (23.8, 21.8, 22.4),
)
UNIT, HOP, BACKLOG = 0.615, 1.75, 1.5
WINDOW = 3.05


def onward(n, d, far):
    if d == 0:
        return [1, -1]
    if d < n // 2:
        return [-1] if d + 1 < n // 2 or far == -1 else []
    if d > n // 2:
        return [1] if d - 1 > n // 2 or far == 1 else []
    return []


def parity(k):
    return 1 if k % 2 == 0 else -1


def sends_of(p):
    color, axis, rest = p[0], p[1], p[2:]
    out = []
    if color == "A" and axis == "y":
        (dy,) = rest
        out += [("y", m, 1, ("A", "y", (dy - m) % 4)) for m in onward(4, dy, 1)]
        out += [("x", m, 1, ("A", "x", dy, -m % 4)) for m in (1, -1)]
    elif color == "A" and axis == "x":
        dy, dx = rest
        out += [("x", m, 1, ("A", "x", dy, (dx - m) % 4)) for m in onward(4, dx, parity(dy))]
    elif color == "A":
        dz, dy = rest
        out += [("z", m, 4, ("A", "z", (dz - m) % 8, dy)) for m in onward(8, dz, parity(dy))]
    elif axis == "z":
        (dz,) = rest
        far = 1 if color == "B" else -1
        out += [("z", m, 1, (color, "z", (dz - m) % 8)) for m in onward(8, dz, far)]
        second = "y" if color == "B" else "x"
        out += [(second, m, 1, (color, second, dz, -m % 4)) for m in (1, -1)]
    else:
        dz, d = rest
        last = (color, axis) in (("B", "x"), ("C", "y"))
        size = 4 if last else 1
        out += [(axis, m, size, (color, axis, dz, (d - m) % 4)) for m in onward(4, d, parity(dz))]
    return out


def launch_of(p):
    color, axis = p[0], p[1]
    if color == "A" and axis != "z":
        return ("A", "z", 0, p[2])
    if color == "B" and axis != "x":
        return ("B", "x", p[2], 0)
    if color == "C" and axis != "y":
        return ("C", "y", p[2], 0)
    return None


def parts_of(launch):
    color, _, a, b = launch
    if color == "A":
        return [("A", "y", b)] + [("A", "x", b, k) for k in (1, 2, 3)]
    if color == "B":
        return [("B", "z", a)] + [("B", "y", a, k) for k in (1, 2, 3)]
    return [("C", "z", a)] + [("C", "x", a, k) for k in (1, 2, 3)]


def window_of(p):
    return 0 if p[0] == "A" and p[1] != "z" else p[2]


def pieces_of_chunk(dz, color):
    last = (("A", "z"), ("B", "x"), ("C", "y"))[color]
    return [(*last, dz, k) for k in range(4)]


def plan(preps, chunks=None):
    due = {}

    def latest(p):
        if p not in due:
            dz = window_of(p)
            k = DEADLINE[dz][{"A": 0, "B": 1, "C": 2}[p[0]]]
            ahead = sends_of(p)
            launch = launch_of(p)
            if launch:
                ahead = ahead + sends_of(launch)
            for _, _, size, q in ahead:
                k = min(k, latest(q) - HOP - size * UNIT - 0.3)
            due[p] = k
        return due[p]

    free = {(a, m): 0.0 for a in "xyz" for m in (1, -1)}
    waiting = {k: [] for k in free}
    have, steps, flying = set(), [], []
    count = 0
    now = 0.0

    def offer(sends):
        nonlocal count
        for axis, m, size, q in sends:
            heapq.heappush(waiting[axis, m], (latest(q) - size * UNIT, count, size, q))
            count += 1

    def pump():
        nonlocal count
        for link in free:
            while waiting[link] and free[link] - now < BACKLOG:
                _, _, size, q = heapq.heappop(waiting[link])
                free[link] = max(free[link], now) + size * UNIT
                heapq.heappush(flying, (free[link] + HOP, count, q))
                count += 1
                steps.append(("send", link[0], link[1], q))

    def take(p):
        have.add(p)
        offer(sends_of(p))
        launch = launch_of(p)
        if launch and launch not in have and all(q in have for q in parts_of(launch)):
            have.add(launch)
            offer(sends_of(launch))

    def blocked():
        return any(p[0][0] == "other" for p in preps)

    for p in (("A", "y", 0), ("B", "z", 0), ("C", "z", 0)):
        take(p)
    pump()
    arrived = {}
    left = list(range(WINDOWS)) if chunks else []
    preps = list(preps)
    while flying or left or preps:
        if flying and flying[0][0] <= now:
            _, _, q = heapq.heappop(flying)
            steps.append(("wait", q))
            arrived[q] = now
            take(q)
            pump()
            now += 0.03
            continue
        if preps and now >= preps[0][1]:
            name, _, cost = preps.pop(0)
            steps.append(("prep", name))
            now += cost
            pump()
            continue
        ready = [] if blocked() else [w for w in left if all(
            q in have for chunk in chunks[4 * w:4 * w + 4] for q in pieces_of_chunk(*chunk))]
        if ready:
            steps.append(("window", ready[0]))
            left.remove(ready[0])
            now += WINDOW
            pump()
            continue
        nxt = [flying[0][0]] if flying else []
        if preps:
            nxt.append(preps[0][1])
        now = max(now, min(nxt))
    if chunks is None:
        every = [(dz, color) for dz in range(NZ) for color in range(COLORS)]
        return sorted(every, key=lambda t: max(arrived.get(q, 0.0) for q in pieces_of_chunk(*t)))
    return steps, now


PREPS = (
    [(("limits", 0), 0.2, 0.3), (("places", 0), 0.8, 0.4)]
    + [(("own", k), 3.0, 0.3) for k in range(2)]
    + [(("other", k), 11.0, 0.3) for k in range(2)]
    + [(("mask", 0), 16.0, 0.1), (("mask", 1), 32.0, 0.1)]
)
CHUNKS = plan(PREPS)
STEPS, _ = plan(PREPS, CHUNKS)
SPOT = {chunk: k for k, chunk in enumerate(CHUNKS)}
TRANSFERS = [s[3] for s in STEPS if s[0] == "send"]


def shared_semaphores(steps):
    sent = {s[3]: k for k, s in enumerate(steps) if s[0] == "send"}
    waited = {s[1]: k for k, s in enumerate(steps) if s[0] == "wait"}
    links = {}
    for s in steps:
        if s[0] == "send":
            links.setdefault(s[1:3], []).append(s[3])
    number, count = {}, 0
    for (axis, m), queue in links.items():
        slots = []
        for q in queue:
            for slot in slots:
                if any(sent[r] > waited[slot[1]] and waited[r] < sent[q] for r in links[axis, -m]):
                    break
            else:
                slot = [count, None]
                slots.append(slot)
                count += 1
            slot[1] = q
            number[q] = slot[0]
    return number, count


NUMBER, SEMAPHORES = shared_semaphores(STEPS)
LARGE = [q for q in TRANSFERS if q[:2] in (("A", "z"), ("B", "x"), ("C", "y"))]
SMALL = [q for q in TRANSFERS if q not in LARGE]
WHOLE = len(SMALL) // 4 * 4
GROUP = {q: 0 for q in LARGE}
GROUP.update({q: 1 if k < WHOLE else 2 + k - WHOLE for k, q in enumerate(SMALL)})


def merge(parts):
    peak = parts[0][0]
    for p in parts[1:]:
        peak = jnp.maximum(peak, p[0])
    total = jnp.zeros_like(peak)
    moment = jnp.zeros_like(peak)
    for m, t, mo in parts:
        shift = m - peak
        ratio = jnp.exp(shift)
        total = total + ratio * t
        moment = moment + ratio * (mo + t * shift)
    return peak, total, moment


def kernel(hid_ref, lm_ref, pos_ref, lim_ref, mask_ref, ent_ref, mean_ref,
           held, weight, stage, hstage, pstage, logits, small, mask_in, table, lim_win, pos_col,
           wstat, stat, from_z, plane, from_plane, ents, masks,
           send_sem, recv_sem, hx_sem, w_sem, mz_sem, my_sem, rz_sem, rp_sem, re_sem, copy_sem):
    z, y, x, c = (lax.axis_index(a) for a in AXES)
    here = {"z": z, "y": y, "x": x, "c": c}

    def device(**moved):
        return tuple(lax.rem(here[a] + moved[a], SIZE[a]) if a in moved and a != "c" else
                     (1 - c if a in moved else here[a]) for a in AXES)

    own_w = pltpu.make_async_copy(lm_ref, stage.at[0], copy_sem.at[0])
    own_h = pltpu.make_async_copy(hid_ref, hstage, copy_sem.at[1])
    own_h.start()
    own_w.start()
    given = [pltpu.make_async_copy(lim_ref, small.at[0], copy_sem.at[2]),
             pltpu.make_async_copy(pos_ref, small.at[1], copy_sem.at[3]),
             pltpu.make_async_copy(mask_ref, mask_in, copy_sem.at[4])]
    for copy in given:
        copy.start()

    barrier = pltpu.get_barrier_semaphore()
    near = [device(**{a: d}) for a in "zyx" for d in (1, SIZE[a] - 1)] + [device(c=1)]
    for who in near:
        pl.semaphore_signal(barrier, inc=1, device_id=who, device_id_type=MESH)
    with jax.named_scope("T_barrier"):
        pl.semaphore_wait(barrier, len(near))

    with jax.named_scope("T_ownh"):
        own_h.wait()
    swap = pltpu.make_async_remote_copy(
        src_ref=hstage.at[pl.ds(pl.multiple_of((1 - c) * HALF, RB), HALF), :], dst_ref=pstage,
        send_sem=hx_sem.at[0], recv_sem=hx_sem.at[1], device_id=device(c=1), device_id_type=MESH)
    swap.start()
    give_w = pltpu.make_async_remote_copy(
        src_ref=lm_ref, dst_ref=stage.at[1],
        send_sem=w_sem.at[0], recv_sem=w_sem.at[1], device_id=device(c=1), device_id_type=MESH)

    def feature(dx):
        return pl.ds(pl.multiple_of(lax.rem(x + dx, NX) * FEAT, 128), FEAT)

    mine = hstage[pl.ds(pl.multiple_of(c * HALF, RB), HALF), :].astype(jnp.float32)
    with jax.named_scope("T_swap"):
        swap.wait_recv()
    theirs = pstage[...].astype(jnp.float32)
    first = c == 0
    left = jnp.where(first, mine, theirs)
    right = jnp.where(first, theirs, mine)
    both = jnp.concatenate([left, right], axis=1).astype(jnp.bfloat16)
    for k in range(COLORS):
        held[pl.ds(SPOT[0, k] * CHUNK, RB), feature(0)] = both[k * RB:(k + 1) * RB]

    def rows_of(p):
        color, axis = "ABC".index(p[0]), p[1]
        dz = window_of(p)
        if p[:2] == ("B", "x"):
            return pl.ds(SPOT[dz, color] * CHUNK, CHUNK)
        if axis == "z":
            dy = p[3] if color == 0 else 0
        elif axis == "y":
            dy = p[2] if color == 0 else p[3]
        else:
            dy = p[2] if color == 0 else 0
        return pl.ds(SPOT[dz, color] * CHUNK + dy * RB, RB)

    def place(p):
        if p[:2] in (("A", "z"), ("C", "y")):
            return held.at[rows_of(p), :]
        return held.at[rows_of(p), feature(p[-1] if p[1] == "x" else 0)]

    def transfer(q, axis, m):
        n = SIZE[axis]
        if axis == "x":
            src = dst = held.at[rows_of(q), feature(q[-1] + m + NX)]
        else:
            at = {("A", "y"): 2, ("A", "z"): 2, ("B", "z"): 2, ("C", "z"): 2}.get(q[:2], 3)
            src = place(q[:at] + ((q[at] + m) % n,) + q[at + 1:])
            dst = place(q)
        return pltpu.make_async_remote_copy(
            src_ref=src, dst_ref=dst, send_sem=send_sem.at[GROUP[q]], recv_sem=recv_sem.at[NUMBER[q]],
            device_id=device(**{axis: m % n}), device_id_type=MESH)

    started = {}
    lanes = lax.broadcasted_iota(jnp.int32, (128, 128), 1)

    lane_of = lax.broadcasted_iota(jnp.int32, (8, LANES), 1)
    lane_chunk = lane_of // CHUNK

    def limits():
        for copy in given:
            copy.wait()
        masks[0, 0] = jnp.zeros((1, 128), jnp.float32)
        masks[0, 0, :, 0:TOK] = mask_in[...].astype(jnp.float32)
        row = lax.broadcasted_iota(jnp.int32, (3 * 128, LANES), 0)
        column = lax.broadcasted_iota(jnp.int32, (3 * 128, LANES), 1)
        color, dy, i = column // CHUNK, column % CHUNK // RB, column % RB
        want = lax.rem(y + dy, NY) * TOK + c * HALF + color * RB + i
        pick = jnp.where((row == want) & (color < COLORS), 1.0, 0.0).astype(jnp.bfloat16)
        for k in range(2):
            given_rows = jnp.concatenate(
                [small[k, pl.ds(j, NZ, stride=3), :] for j in range(3)], axis=1)
            found = jnp.zeros((NZ, LANES), jnp.float32)
            for shift in (14, 7, 0):
                digit = lax.bitwise_and(lax.shift_right_logical(given_rows, shift), 127)
                digit = digit.astype(jnp.float32).astype(jnp.bfloat16)
                found = found * 128.0 + jnp.dot(digit, pick, preferred_element_type=jnp.float32)
            table[k] = found

    def places():
        for w in range(WINDOWS):
            line = jnp.zeros((8, LANES), jnp.float32)
            for j in range(4):
                dz, color = CHUNKS[4 * w + j]
                source = jnp.broadcast_to(table[0, pl.ds(lax.rem(z + dz, NZ), 1), :], (8, LANES))
                if j != color:
                    source = pltpu.roll(source, (j - color) * CHUNK % LANES, 1)
                line = jnp.where(lane_chunk == j, source, line)
            lim_win[w] = line[0:1].astype(jnp.int32)
        pos_col[...] = jnp.broadcast_to(table[1, pl.ds(z, 1), :], (128, LANES)).T

    def settle(which, k):
        def one(r, carry):
            at = pl.ds(pl.multiple_of(r * 256, 128), 256)
            weight[which, 0:WID, at] = stage[which, :, at]
            return carry

        lax.fori_loop(7 * k, 7 * k + 7, one, 0)

    def mask_z(dz):
        return pltpu.make_async_remote_copy(
            src_ref=masks.at[0, 0], dst_ref=masks.at[8 - dz, 0], send_sem=mz_sem.at[0],
            recv_sem=mz_sem.at[1], device_id=device(z=dz), device_id_type=MESH)

    def mask_y(dy):
        return pltpu.make_async_remote_copy(
            src_ref=masks.at[:, 0], dst_ref=masks.at[:, 4 - dy], send_sem=my_sem.at[0],
            recv_sem=my_sem.at[1], device_id=device(y=dy), device_id_type=MESH)

    def whole(ref, sems):
        return pltpu.make_async_remote_copy(
            src_ref=ref, dst_ref=ref, send_sem=sems.at[0], recv_sem=sems.at[1],
            device_id=device(z=1), device_id_type=MESH)

    all_mask_z = whole(masks.at[1:NZ, 0], mz_sem)
    all_mask_y = whole(masks.at[:, 1:NY], my_sem)
    all_stat = whole(from_z.at[1:NZ], rz_sem)
    all_plane = whole(from_plane.at[1:NY * NX], rp_sem)
    all_ents = whole(ents.at[1:2 * NZ], re_sem)

    def prep(name, k):
        if name == "limits":
            limits()
        elif name == "places":
            places()
        elif name == "own":
            if k == 0:
                own_w.wait()
            settle(0, k)
        elif name == "other":
            if k == 0:
                give_w.wait_recv()
            settle(1, k)
        elif k == 0:
            for dz in range(1, NZ):
                mask_z(dz).start()
        else:
            all_mask_z.wait_recv()
            for dy in range(1, NY):
                mask_y(dy).start()

    number = (z * NY + y) * (2 * NX) + x * 2
    starts = ((number + c) * WID, (number + 1 - c) * WID)
    depth = lax.broadcasted_iota(jnp.int32, (PAD, LANES), 0)

    def multiply(w, slot):
        for k in range(2):
            logits[slot, k] = lax.dot_general(
                weight[k], held[w * LANES:(w + 1) * LANES, :], (((1,), (1,)), ((), ())),
                preferred_element_type=jnp.float32)

    def reduce_rows(w, slot):
        limit = lim_win[w]
        peak = jnp.full((1, LANES), NEG, jnp.float32)
        for k in range(2):
            bound = jnp.minimum(limit - starts[k], WID)
            logits[slot, k] = jnp.where(depth < bound, logits[slot, k], NEG)
            peak = jnp.maximum(peak, jnp.max(logits[slot, k], axis=0, keepdims=True))
        total = jnp.zeros((1, LANES), jnp.float32)
        moment = jnp.zeros((1, LANES), jnp.float32)
        for k in range(2):
            shifted = logits[slot, k] - peak
            e = jnp.exp(shifted)
            total = total + jnp.sum(e, axis=0, keepdims=True)
            moment = moment + jnp.sum(e * shifted, axis=0, keepdims=True)
        wstat[w] = jnp.concatenate([peak, total, moment, jnp.zeros((5, LANES), jnp.float32)], axis=0)
        reduced.append(w)
        for dz in range(NZ):
            spots = [SPOT[dz, color] for color in range(COLORS)]
            if any(spot // 4 == w for spot in spots) and all(spot // 4 in reduced for spot in spots):
                line = jnp.zeros((8, LANES), jnp.float32)
                for color, spot in enumerate(spots):
                    source = wstat[spot // 4]
                    if spot % 4 != color:
                        source = pltpu.roll(source, (color - spot % 4) * CHUNK % LANES, 1)
                    line = jnp.where(lane_chunk == color, source, line)
                for k in range(3):
                    stat[dz, k] = line[k:k + 1]
                if dz:
                    stat_copy(dz).start()

    def stat_copy(dz):
        return pltpu.make_async_remote_copy(
            src_ref=stat.at[dz], dst_ref=from_z.at[8 - dz], send_sem=rz_sem.at[0],
            recv_sem=rz_sem.at[1], device_id=device(z=dz), device_id_type=MESH)

    done, reduced = [], []

    def window(dz):
        if done:
            reduce_rows(done[-1], len(done) % 2)
        if dz is None:
            return
        done.append(dz)
        multiply(dz, len(done) % 2)

    first_send = True
    for step in STEPS:
        if step[0] == "send":
            _, axis, m, q = step
            started[q] = transfer(q, axis, m)
            started[q].start()
        else:
            if first_send:
                give_w.start()
                first_send = False
            if step[0] == "wait":
                started[step[1]].wait_recv()
            elif step[0] == "prep":
                prep(*step[1])
            else:
                window(step[1])
    with jax.named_scope("T_last"):
        window(None)

    with jax.named_scope("T_zround"):
        all_stat.wait_recv()
    parts = [tuple(stat[0, k] for k in range(3))]
    parts += [tuple(from_z[dz, k] for k in range(3)) for dz in range(1, NZ)]
    merged = merge(parts)
    for k in range(3):
        plane[k] = merged[k]

    spots = [(dy, dx) for dy in range(NY) for dx in range(NX) if dy or dx]

    def plane_copy(dy, dx):
        back = (NY - dy) % NY * NX + (NX - dx) % NX
        return pltpu.make_async_remote_copy(
            src_ref=plane, dst_ref=from_plane.at[back], send_sem=rp_sem.at[0],
            recv_sem=rp_sem.at[1], device_id=device(y=dy, x=dx), device_id_type=MESH)

    for dy, dx in spots:
        plane_copy(dy, dx).start()
    all_mask_y.wait_recv()
    with jax.named_scope("T_planeround"):
        all_plane.wait_recv()
    groups = []
    for dy in range(NY):
        parts = [tuple(from_plane[dy * NX + dx, k] for k in range(3)) for dx in range(NX) if dy or dx]
        group = merge(parts if dy else [merged] + parts)
        if dy:
            lines = jnp.concatenate([*group, jnp.zeros((5, LANES), jnp.float32)], axis=0)
            ahead = pltpu.roll(lines, dy * RB, 1)
            around = pltpu.roll(lines, (dy * RB - CHUNK) % LANES, 1)
            lines = jnp.where(lane_of % CHUNK >= dy * RB, ahead, around)
            group = tuple(lines[k:k + 1] for k in range(3))
        groups.append(group)
    peak, total, moment = merge(groups)
    entropy = jnp.log(total) - moment / total

    masked = jnp.zeros((1, 128), jnp.float32)
    found = []
    column = jnp.broadcast_to(entropy, (128, LANES)).T[:COLORS * CHUNK]
    for k in range(2):
        owner = jnp.where(c == 0, 2 * z + k, 31 - 2 * z - k)
        line = lanes[:1]
        spot = jnp.where(line < TOK, owner * TOK + line, -1).astype(jnp.float32)
        here_e = jnp.where(pos_col[0:COLORS * CHUNK, :] == spot, column, 0.0)
        here_e = jnp.sum(here_e, axis=0, keepdims=True)
        found.append(here_e)
        dz = lax.rem(owner // NY - z + NZ, NZ)
        dy = lax.rem(lax.rem(owner, NY) - y + NY, NY)
        masked = masked + here_e * masks[dz, dy]
    masked = jnp.sum(masked, axis=1, keepdims=True)
    lane = lanes[:1]
    for k in range(2):
        ents[0, k] = jnp.where(lane < TOK, found[k], masked if k == 0 else 0.0)

    others = [(dz, other) for dz in range(NZ) for other in range(2) if dz or other]

    def ent_copy(dz, other):
        target = device(z=dz, c=1) if other else device(z=dz)
        return pltpu.make_async_remote_copy(
            src_ref=ents.at[0], dst_ref=ents.at[(NZ - dz) % NZ * 2 + other], send_sem=re_sem.at[0],
            recv_sem=re_sem.at[1], device_id=target, device_id_type=MESH)

    for dz, other in others:
        ent_copy(dz, other).start()

    started_count = jnp.sum(jnp.sum(masks[...].reshape(NZ * NY, 128), axis=0, keepdims=True), axis=1, keepdims=True)
    for group, rows in ((0, len(LARGE) * RB), (1, WHOLE // 4 * RB)):
        pltpu.make_async_remote_copy(
            src_ref=held.at[0:rows, :], dst_ref=held.at[0:rows, :], send_sem=send_sem.at[group],
            recv_sem=recv_sem.at[0], device_id=device(z=1), device_id_type=MESH).wait_send()
    for q in SMALL[WHOLE:]:
        started[q].wait_send()
    swap.wait_send()
    give_w.wait_send()
    all_mask_z.wait_send()
    all_mask_y.wait_send()
    all_stat.wait_send()
    all_plane.wait_send()

    with jax.named_scope("T_entround"):
        all_ents.wait_recv()
    total_masked = jnp.sum(ents[:, 0].reshape(2 * NZ, 128), axis=0, keepdims=True)
    total_masked = jnp.sum(jnp.where(lane == TOK, total_masked, 0.0), axis=1, keepdims=True)
    mean = total_masked / jnp.maximum(started_count, 1.0)
    mean_ref[...] = jnp.broadcast_to(mean, (1, 128))
    mine_s = z * NY + y
    index = jnp.where(z < NZ // 2, mine_s, 31 - mine_s)
    dz = lax.rem(index // 2 - z + NZ, NZ)
    other = jnp.where(z < NZ // 2, c, 1 - c)
    ent_ref[...] = ents[dz * 2 + other, lax.rem(index, 2)][:, 0:TOK]
    all_ents.wait_send()


def local(hidden, lm_head, positions, vocab_limits, loss_mask):
    f32, bf16 = jnp.float32, jnp.bfloat16
    dma = pltpu.SemaphoreType.DMA
    any_space = pl.BlockSpec(memory_space=pl.ANY)
    vmem = pl.BlockSpec(memory_space=pltpu.VMEM)
    ent, mean = pl.pallas_call(
        kernel,
        out_shape=(jax.ShapeDtypeStruct((1, TOK), f32), jax.ShapeDtypeStruct((1, 128), f32)),
        in_specs=[any_space] * 5,
        out_specs=(vmem, vmem),
        scratch_shapes=[
            pltpu.VMEM((NZ * COLORS * CHUNK, D), bf16),
            pltpu.VMEM((2, PAD, D), bf16),
            pltpu.VMEM((2, WID, D), bf16),
            pltpu.VMEM((TOK, FEAT // 2), bf16),
            pltpu.VMEM((HALF, FEAT // 2), bf16),
            pltpu.VMEM((2, 2, PAD, LANES), f32),
            pltpu.VMEM((2, 24, 128), jnp.int32),
            pltpu.VMEM((1, TOK), jnp.int32),
            pltpu.VMEM((2, NZ, LANES), f32),
            pltpu.VMEM((WINDOWS, 1, LANES), jnp.int32),
            pltpu.VMEM((LANES, 128), f32),
            pltpu.VMEM((WINDOWS, 8, LANES), f32),
            pltpu.VMEM((NZ, 3, 1, 256), f32),
            pltpu.VMEM((NZ, 3, 1, 256), f32),
            pltpu.VMEM((3, 1, 256), f32),
            pltpu.VMEM((NY * NX, 3, 1, 256), f32),
            pltpu.VMEM((2 * NZ, 2, 1, 128), f32),
            pltpu.VMEM((NZ, NY, 1, 128), f32),
            dma((2 + len(SMALL) - WHOLE,)), dma((SEMAPHORES,)), *[dma((2,))] * 7, dma((5,)),
        ],
        compiler_params=pltpu.CompilerParams(
            collective_id=0, has_side_effects=True, vmem_limit_bytes=62 * 2**20),
    )(hidden, lm_head.T, positions.reshape(24, 128), vocab_limits.reshape(24, 128), loss_mask.reshape(1, TOK))
    return ent.reshape(TOK), mean[0, 0]


def solution(mesh):
    torus = Mesh(mesh.devices.reshape(NZ, NY, NX, 2), AXES)
    in_specs = (P(("z", "y"), ("x", "c")), P(None, AXES), P(), P(), P(("z", "y")))
    return jax.shard_map(local, mesh=torus, in_specs=in_specs, out_specs=(P(("z", "y")), P()), check_vma=False)
```

```python
import heapq

import jax
import jax.numpy as jnp
from jax import lax
from jax.experimental import pallas as pl
from jax.experimental.pallas import tpu as pltpu
from jax.sharding import Mesh
from jax.sharding import PartitionSpec as P

NZ, NY, NX = 8, 4, 4
SIZE = {"z": NZ, "y": NY, "x": NX}
AXES = ("z", "y", "x", "c")
MESH = pl.DeviceIdType.MESH
HALF, RB, COLORS = 48, 16, 3
TOK = 96
D, FEAT = 3584, 896
WID, PAD = 594, 608
CHUNK, LANES = 64, 256
WINDOWS = NZ * COLORS * CHUNK // LANES
NEG = -1e30
DEADLINE = (
    (3.9, -0.7, 0.5),
    (12.3, 9.6, 12.3),
    (17.2, 16.7, 14.0),
    (16.6, 15.8, 16.5),
    (21.7, 22.0, 23.4),
    (12.3, 23.1, 18.4),
    (15.1, 15.7, 15.8),
    (12.2, 15.3, 13.4),
)
UNIT, HOP, BACKLOG = 0.615, 2.5, 2
WINDOW = 3.05


def onward(n, d, far):
    if d == 0:
        return [1, -1]
    if d < n // 2:
        return [-1] if d + 1 < n // 2 or far == -1 else []
    if d > n // 2:
        return [1] if d - 1 > n // 2 or far == 1 else []
    return []


def parity(k):
    return 1 if k % 2 == 0 else -1


def sends_of(p):
    color, axis, rest = p[0], p[1], p[2:]
    out = []
    if color == "A" and axis == "y":
        (dy,) = rest
        out += [("y", m, 1, ("A", "y", (dy - m) % 4)) for m in onward(4, dy, 1)]
        out += [("x", m, 1, ("A", "x", dy, -m % 4)) for m in (1, -1)]
    elif color == "A" and axis == "x":
        dy, dx = rest
        out += [("x", m, 1, ("A", "x", dy, (dx - m) % 4)) for m in onward(4, dx, parity(dy))]
    elif color == "A":
        dz, dy = rest
        out += [("z", m, 4, ("A", "z", (dz - m) % 8, dy)) for m in onward(8, dz, parity(dy))]
    elif axis == "z":
        (dz,) = rest
        far = 1 if color == "B" else -1
        out += [("z", m, 1, (color, "z", (dz - m) % 8)) for m in onward(8, dz, far)]
        second = "y" if color == "B" else "x"
        out += [(second, m, 1, (color, second, dz, -m % 4)) for m in (1, -1)]
    else:
        dz, d = rest
        last = (color, axis) in (("B", "x"), ("C", "y"))
        size = 4 if last else 1
        out += [(axis, m, size, (color, axis, dz, (d - m) % 4)) for m in onward(4, d, parity(dz))]
    return out


def launch_of(p):
    color, axis = p[0], p[1]
    if color == "A" and axis != "z":
        return ("A", "z", 0, p[2])
    if color == "B" and axis != "x":
        return ("B", "x", p[2], 0)
    if color == "C" and axis != "y":
        return ("C", "y", p[2], 0)
    return None


def parts_of(launch):
    color, _, a, b = launch
    if color == "A":
        return [("A", "y", b)] + [("A", "x", b, k) for k in (1, 2, 3)]
    if color == "B":
        return [("B", "z", a)] + [("B", "y", a, k) for k in (1, 2, 3)]
    return [("C", "z", a)] + [("C", "x", a, k) for k in (1, 2, 3)]


def window_of(p):
    return 0 if p[0] == "A" and p[1] != "z" else p[2]


def pieces_of_chunk(dz, color):
    last = (("A", "z"), ("B", "x"), ("C", "y"))[color]
    return [(*last, dz, k) for k in range(4)]


def plan(preps, chunks=None):
    due = {}

    def latest(p):
        if p not in due:
            dz = window_of(p)
            k = DEADLINE[dz][{"A": 0, "B": 1, "C": 2}[p[0]]]
            ahead = sends_of(p)
            launch = launch_of(p)
            if launch:
                ahead = ahead + sends_of(launch)
            for _, _, size, q in ahead:
                k = min(k, latest(q) - HOP - size * UNIT - 0.3)
            due[p] = k
        return due[p]

    free = {(a, m): 0.0 for a in "xyz" for m in (1, -1)}
    waiting = {k: [] for k in free}
    have, steps, flying = set(), [], []
    count = 0
    now = 0.0

    def offer(sends):
        nonlocal count
        for axis, m, size, q in sends:
            heapq.heappush(waiting[axis, m], (latest(q) - size * UNIT, count, size, q))
            count += 1

    def pump():
        nonlocal count
        for link in free:
            while waiting[link] and free[link] - now < BACKLOG:
                _, _, size, q = heapq.heappop(waiting[link])
                free[link] = max(free[link], now) + size * UNIT
                heapq.heappush(flying, (free[link] + HOP, count, q))
                count += 1
                steps.append(("send", link[0], link[1], q))

    def take(p):
        have.add(p)
        offer(sends_of(p))
        launch = launch_of(p)
        if launch and launch not in have and all(q in have for q in parts_of(launch)):
            have.add(launch)
            offer(sends_of(launch))

    def blocked():
        return any(p[0][0] == "other" for p in preps)

    for p in (("A", "y", 0), ("B", "z", 0), ("C", "z", 0)):
        take(p)
    pump()
    arrived = {}
    left = list(range(WINDOWS)) if chunks else []
    preps = list(preps)
    while flying or left or preps:
        if flying and flying[0][0] <= now:
            _, _, q = heapq.heappop(flying)
            steps.append(("wait", q))
            arrived[q] = now
            take(q)
            pump()
            now += 0.03
            continue
        if preps and now >= preps[0][1]:
            name, _, cost = preps.pop(0)
            steps.append(("prep", name))
            now += cost
            pump()
            continue
        ready = [] if blocked() else [w for w in left if all(
            q in have for chunk in chunks[4 * w:4 * w + 4] for q in pieces_of_chunk(*chunk))]
        if ready:
            steps.append(("window", ready[0]))
            left.remove(ready[0])
            now += WINDOW
            pump()
            continue
        nxt = [flying[0][0]] if flying else []
        if preps:
            nxt.append(preps[0][1])
        now = max(now, min(nxt))
    if chunks is None:
        every = [(dz, color) for dz in range(NZ) for color in range(COLORS)]
        return sorted(every, key=lambda t: max(arrived.get(q, 0.0) for q in pieces_of_chunk(*t)))
    return steps, now


PREPS = (
    [(("limits", 0), 0.2, 0.3), (("places", 0), 0.8, 0.4)]
    + [(("own", k), 3.0, 0.3) for k in range(2)]
    + [(("other", k), 11.0, 0.3) for k in range(2)]
    + [(("mask", 0), 16.0, 0.1), (("mask", 1), 32.0, 0.1)]
)
CHUNKS = plan(PREPS)
STEPS, _ = plan(PREPS, CHUNKS)
SPOT = {chunk: k for k, chunk in enumerate(CHUNKS)}
TRANSFERS = [s[3] for s in STEPS if s[0] == "send"]


def shared_semaphores(steps):
    sent = {s[3]: k for k, s in enumerate(steps) if s[0] == "send"}
    waited = {s[1]: k for k, s in enumerate(steps) if s[0] == "wait"}
    links = {}
    for s in steps:
        if s[0] == "send":
            links.setdefault(s[1:3], []).append(s[3])
    number, count = {}, 0
    for (axis, m), queue in links.items():
        slots = []
        for q in queue:
            for slot in slots:
                if any(sent[r] > waited[slot[1]] and waited[r] < sent[q] for r in links[axis, -m]):
                    break
            else:
                slot = [count, None]
                slots.append(slot)
                count += 1
            slot[1] = q
            number[q] = slot[0]
    return number, count


NUMBER, SEMAPHORES = shared_semaphores(STEPS)
LARGE = [q for q in TRANSFERS if q[:2] in (("A", "z"), ("B", "x"), ("C", "y"))]
SMALL = [q for q in TRANSFERS if q not in LARGE]
WHOLE = len(SMALL) // 4 * 4
GROUP = {q: 0 for q in LARGE}
GROUP.update({q: 1 if k < WHOLE else 2 + k - WHOLE for k, q in enumerate(SMALL)})


def merge(parts):
    peak = parts[0][0]
    for p in parts[1:]:
        peak = jnp.maximum(peak, p[0])
    total = jnp.zeros_like(peak)
    moment = jnp.zeros_like(peak)
    for m, t, mo in parts:
        shift = m - peak
        ratio = jnp.exp(shift)
        total = total + ratio * t
        moment = moment + ratio * (mo + t * shift)
    return peak, total, moment


def kernel(hid_ref, lm_ref, pos_ref, lim_ref, mask_ref, ent_ref, mean_ref,
           held, weight, stage, hstage, pstage, logits, small, mask_in, table, lim_win, pos_col,
           wstat, stat, from_z, plane, from_plane, ents, masks,
           send_sem, recv_sem, hx_sem, w_sem, mz_sem, my_sem, rz_sem, rp_sem, re_sem, copy_sem):
    z, y, x, c = (lax.axis_index(a) for a in AXES)
    here = {"z": z, "y": y, "x": x, "c": c}

    def device(**moved):
        return tuple(lax.rem(here[a] + moved[a], SIZE[a]) if a in moved and a != "c" else
                     (1 - c if a in moved else here[a]) for a in AXES)

    own_w = pltpu.make_async_copy(lm_ref, stage.at[0], copy_sem.at[0])
    own_h = pltpu.make_async_copy(hid_ref, hstage, copy_sem.at[1])
    own_h.start()
    own_w.start()
    given = [pltpu.make_async_copy(lim_ref, small.at[0], copy_sem.at[2]),
             pltpu.make_async_copy(pos_ref, small.at[1], copy_sem.at[3]),
             pltpu.make_async_copy(mask_ref, mask_in, copy_sem.at[4])]
    for copy in given:
        copy.start()

    barrier = pltpu.get_barrier_semaphore()
    near = [device(**{a: d}) for a in "zyx" for d in (1, SIZE[a] - 1)] + [device(c=1)]
    for who in near:
        pl.semaphore_signal(barrier, inc=1, device_id=who, device_id_type=MESH)
    with jax.named_scope("T_barrier"):
        pl.semaphore_wait(barrier, len(near))

    with jax.named_scope("T_ownh"):
        own_h.wait()
    swap = pltpu.make_async_remote_copy(
        src_ref=hstage.at[pl.ds(pl.multiple_of((1 - c) * HALF, RB), HALF), :], dst_ref=pstage,
        send_sem=hx_sem.at[0], recv_sem=hx_sem.at[1], device_id=device(c=1), device_id_type=MESH)
    swap.start()
    give_w = pltpu.make_async_remote_copy(
        src_ref=lm_ref, dst_ref=stage.at[1],
        send_sem=w_sem.at[0], recv_sem=w_sem.at[1], device_id=device(c=1), device_id_type=MESH)

    def feature(dx):
        return pl.ds(pl.multiple_of(lax.rem(x + dx, NX) * FEAT, 128), FEAT)

    mine = hstage[pl.ds(pl.multiple_of(c * HALF, RB), HALF), :].astype(jnp.float32)
    with jax.named_scope("T_swap"):
        swap.wait_recv()
    theirs = pstage[...].astype(jnp.float32)
    first = c == 0
    left = jnp.where(first, mine, theirs)
    right = jnp.where(first, theirs, mine)
    both = jnp.concatenate([left, right], axis=1).astype(jnp.bfloat16)
    for k in range(COLORS):
        held[pl.ds(SPOT[0, k] * CHUNK, RB), feature(0)] = both[k * RB:(k + 1) * RB]

    def rows_of(p):
        color, axis = "ABC".index(p[0]), p[1]
        dz = window_of(p)
        if p[:2] == ("B", "x"):
            return pl.ds(SPOT[dz, color] * CHUNK, CHUNK)
        if axis == "z":
            dy = p[3] if color == 0 else 0
        elif axis == "y":
            dy = p[2] if color == 0 else p[3]
        else:
            dy = p[2] if color == 0 else 0
        return pl.ds(SPOT[dz, color] * CHUNK + dy * RB, RB)

    def place(p):
        if p[:2] in (("A", "z"), ("C", "y")):
            return held.at[rows_of(p), :]
        return held.at[rows_of(p), feature(p[-1] if p[1] == "x" else 0)]

    def transfer(q, axis, m):
        n = SIZE[axis]
        if axis == "x":
            src = dst = held.at[rows_of(q), feature(q[-1] + m + NX)]
        else:
            at = {("A", "y"): 2, ("A", "z"): 2, ("B", "z"): 2, ("C", "z"): 2}.get(q[:2], 3)
            src = place(q[:at] + ((q[at] + m) % n,) + q[at + 1:])
            dst = place(q)
        return pltpu.make_async_remote_copy(
            src_ref=src, dst_ref=dst, send_sem=send_sem.at[GROUP[q]], recv_sem=recv_sem.at[NUMBER[q]],
            device_id=device(**{axis: m % n}), device_id_type=MESH)

    started = {}
    lanes = lax.broadcasted_iota(jnp.int32, (128, 128), 1)

    rows_z = lax.rem(z + NZ // 2, NZ)
    lane_of = lax.broadcasted_iota(jnp.int32, (8, LANES), 1)
    lane_chunk = lane_of // CHUNK

    def limits():
        for copy in given:
            copy.wait()
        masks[0, 0] = jnp.zeros((1, 128), jnp.float32)
        masks[0, 0, :, 0:TOK] = mask_in[...].astype(jnp.float32)
        row = lax.broadcasted_iota(jnp.int32, (3 * 128, LANES), 0)
        column = lax.broadcasted_iota(jnp.int32, (3 * 128, LANES), 1)
        color, dy, i = column // CHUNK, column % CHUNK // RB, column % RB
        want = lax.rem(y + dy, NY) * TOK + c * HALF + color * RB + i
        pick = jnp.where((row == want) & (color < COLORS), 1.0, 0.0).astype(jnp.bfloat16)
        for k in range(2):
            given_rows = jnp.concatenate(
                [small[k, pl.ds(j, NZ, stride=3), :] for j in range(3)], axis=1)
            found = jnp.zeros((NZ, LANES), jnp.float32)
            for shift in (14, 7, 0):
                digit = lax.bitwise_and(lax.shift_right_logical(given_rows, shift), 127)
                digit = digit.astype(jnp.float32).astype(jnp.bfloat16)
                found = found * 128.0 + jnp.dot(digit, pick, preferred_element_type=jnp.float32)
            table[k] = found

    def places():
        for w in range(WINDOWS):
            line = jnp.zeros((8, LANES), jnp.float32)
            for j in range(4):
                dz, color = CHUNKS[4 * w + j]
                source = jnp.broadcast_to(table[0, pl.ds(lax.rem(z + dz, NZ), 1), :], (8, LANES))
                if j != color:
                    source = pltpu.roll(source, (j - color) * CHUNK % LANES, 1)
                line = jnp.where(lane_chunk == j, source, line)
            lim_win[w] = line[0:1].astype(jnp.int32)
        pos_col[...] = jnp.broadcast_to(table[1, pl.ds(rows_z, 1), :], (128, LANES)).T

    def settle(which, k):
        def one(r, carry):
            at = pl.ds(pl.multiple_of(r * 256, 128), 256)
            weight[which, 0:WID, at] = stage[which, :, at]
            return carry

        lax.fori_loop(7 * k, 7 * k + 7, one, 0)

    def mask_z(dz):
        return pltpu.make_async_remote_copy(
            src_ref=masks.at[0, 0], dst_ref=masks.at[8 - dz, 0], send_sem=mz_sem.at[0],
            recv_sem=mz_sem.at[1], device_id=device(z=dz), device_id_type=MESH)

    def mask_y(dy):
        return pltpu.make_async_remote_copy(
            src_ref=masks.at[:, 0], dst_ref=masks.at[:, 4 - dy], send_sem=my_sem.at[0],
            recv_sem=my_sem.at[1], device_id=device(y=dy), device_id_type=MESH)

    def whole(ref, sems):
        return pltpu.make_async_remote_copy(
            src_ref=ref, dst_ref=ref, send_sem=sems.at[0], recv_sem=sems.at[1],
            device_id=device(z=1), device_id_type=MESH)

    all_mask_z = whole(masks.at[1:NZ, 0], mz_sem)
    all_mask_y = whole(masks.at[:, 1:NY], my_sem)
    all_stat = whole(from_z.at[1:NZ], rz_sem)
    all_plane = whole(from_plane.at[1:NY * NX], rp_sem)
    all_ents = whole(ents.at[1:2 * NZ], re_sem)

    def prep(name, k):
        if name == "limits":
            limits()
        elif name == "places":
            places()
        elif name == "own":
            if k == 0:
                own_w.wait()
            settle(0, k)
        elif name == "other":
            if k == 0:
                give_w.wait_recv()
            settle(1, k)
        elif k == 0:
            for dz in range(1, NZ):
                mask_z(dz).start()
        else:
            all_mask_z.wait_recv()
            for dy in range(1, NY):
                mask_y(dy).start()

    number = (z * NY + y) * (2 * NX) + x * 2
    starts = ((number + c) * WID, (number + 1 - c) * WID)
    depth = lax.broadcasted_iota(jnp.int32, (PAD, LANES), 0)

    def multiply(w, slot):
        for k in range(2):
            logits[slot, k] = lax.dot_general(
                weight[k], held[w * LANES:(w + 1) * LANES, :], (((1,), (1,)), ((), ())),
                preferred_element_type=jnp.float32)

    def reduce_rows(w, slot):
        limit = lim_win[w]
        peak = jnp.full((1, LANES), NEG, jnp.float32)
        for k in range(2):
            bound = jnp.minimum(limit - starts[k], WID)
            logits[slot, k] = jnp.where(depth < bound, logits[slot, k], NEG)
            peak = jnp.maximum(peak, jnp.max(logits[slot, k], axis=0, keepdims=True))
        total = jnp.zeros((1, LANES), jnp.float32)
        moment = jnp.zeros((1, LANES), jnp.float32)
        for k in range(2):
            shifted = logits[slot, k] - peak
            e = jnp.exp(shifted)
            total = total + jnp.sum(e, axis=0, keepdims=True)
            moment = moment + jnp.sum(e * shifted, axis=0, keepdims=True)
        wstat[w] = jnp.concatenate([peak, total, moment, jnp.zeros((5, LANES), jnp.float32)], axis=0)
        reduced.append(w)
        for dz in range(NZ):
            spots = [SPOT[dz, color] for color in range(COLORS)]
            if any(spot // 4 == w for spot in spots) and all(spot // 4 in reduced for spot in spots):
                line = jnp.zeros((8, LANES), jnp.float32)
                for color, spot in enumerate(spots):
                    source = wstat[spot // 4]
                    if spot % 4 != color:
                        source = pltpu.roll(source, (color - spot % 4) * CHUNK % LANES, 1)
                    line = jnp.where(lane_chunk == color, source, line)
                for k in range(3):
                    stat[dz, k] = line[k:k + 1]
                if dz != NZ // 2:
                    stat_copy(dz).start()

    def stat_copy(dz):
        ahead = (dz + NZ // 2) % NZ
        return pltpu.make_async_remote_copy(
            src_ref=stat.at[dz], dst_ref=from_z.at[NZ - ahead], send_sem=rz_sem.at[0],
            recv_sem=rz_sem.at[1], device_id=device(z=ahead), device_id_type=MESH)

    done, reduced = [], []

    def window(dz):
        if done:
            reduce_rows(done[-1], len(done) % 2)
        if dz is None:
            return
        done.append(dz)
        multiply(dz, len(done) % 2)

    first_send = True
    for step in STEPS:
        if step[0] == "send":
            _, axis, m, q = step
            started[q] = transfer(q, axis, m)
            started[q].start()
        else:
            if first_send:
                give_w.start()
                first_send = False
            if step[0] == "wait":
                started[step[1]].wait_recv()
            elif step[0] == "prep":
                prep(*step[1])
            else:
                window(step[1])
    with jax.named_scope("T_last"):
        window(None)

    with jax.named_scope("T_zround"):
        all_stat.wait_recv()
    parts = [tuple(stat[NZ // 2, k] for k in range(3))]
    parts += [tuple(from_z[dz, k] for k in range(3)) for dz in range(1, NZ)]
    merged = merge(parts)
    for k in range(3):
        plane[k] = merged[k]

    spots = [(dy, dx) for dy in range(NY) for dx in range(NX) if dy or dx]

    def plane_copy(dy, dx):
        back = (NY - dy) % NY * NX + (NX - dx) % NX
        return pltpu.make_async_remote_copy(
            src_ref=plane, dst_ref=from_plane.at[back], send_sem=rp_sem.at[0],
            recv_sem=rp_sem.at[1], device_id=device(y=dy, x=dx), device_id_type=MESH)

    for dy, dx in spots:
        plane_copy(dy, dx).start()
    all_mask_y.wait_recv()
    with jax.named_scope("T_planeround"):
        all_plane.wait_recv()
    groups = []
    for dy in range(NY):
        parts = [tuple(from_plane[dy * NX + dx, k] for k in range(3)) for dx in range(NX) if dy or dx]
        group = merge(parts if dy else [merged] + parts)
        if dy:
            lines = jnp.concatenate([*group, jnp.zeros((5, LANES), jnp.float32)], axis=0)
            ahead = pltpu.roll(lines, dy * RB, 1)
            around = pltpu.roll(lines, (dy * RB - CHUNK) % LANES, 1)
            lines = jnp.where(lane_of % CHUNK >= dy * RB, ahead, around)
            group = tuple(lines[k:k + 1] for k in range(3))
        groups.append(group)
    peak, total, moment = merge(groups)
    entropy = jnp.log(total) - moment / total

    masked = jnp.zeros((1, 128), jnp.float32)
    found = []
    column = jnp.broadcast_to(entropy, (128, LANES)).T[:COLORS * CHUNK]
    for k in range(2):
        owner = jnp.where(c == 0, 2 * rows_z + k, 31 - 2 * rows_z - k)
        line = lanes[:1]
        spot = jnp.where(line < TOK, owner * TOK + line, -1).astype(jnp.float32)
        here_e = jnp.where(pos_col[0:COLORS * CHUNK, :] == spot, column, 0.0)
        here_e = jnp.sum(here_e, axis=0, keepdims=True)
        found.append(here_e)
        dz = lax.rem(owner // NY - z + NZ, NZ)
        dy = lax.rem(lax.rem(owner, NY) - y + NY, NY)
        masked = masked + here_e * masks[dz, dy]
    masked = jnp.sum(masked, axis=1, keepdims=True)
    lane = lanes[:1]
    for k in range(2):
        ents[0, k] = jnp.where(lane < TOK, found[k], masked if k == 0 else 0.0)

    others = [(dz, other) for dz in range(NZ) for other in range(2) if dz or other]

    def ent_copy(dz, other):
        target = device(z=dz, c=1) if other else device(z=dz)
        return pltpu.make_async_remote_copy(
            src_ref=ents.at[0], dst_ref=ents.at[(NZ - dz) % NZ * 2 + other], send_sem=re_sem.at[0],
            recv_sem=re_sem.at[1], device_id=target, device_id_type=MESH)

    for dz, other in others:
        ent_copy(dz, other).start()

    started_count = jnp.sum(jnp.sum(masks[...].reshape(NZ * NY, 128), axis=0, keepdims=True), axis=1, keepdims=True)
    for group, rows in ((0, len(LARGE) * RB), (1, WHOLE // 4 * RB)):
        pltpu.make_async_remote_copy(
            src_ref=held.at[0:rows, :], dst_ref=held.at[0:rows, :], send_sem=send_sem.at[group],
            recv_sem=recv_sem.at[0], device_id=device(z=1), device_id_type=MESH).wait_send()
    for q in SMALL[WHOLE:]:
        started[q].wait_send()
    swap.wait_send()
    give_w.wait_send()
    all_mask_z.wait_send()
    all_mask_y.wait_send()
    all_stat.wait_send()
    all_plane.wait_send()

    with jax.named_scope("T_entround"):
        all_ents.wait_recv()
    total_masked = jnp.sum(ents[:, 0].reshape(2 * NZ, 128), axis=0, keepdims=True)
    total_masked = jnp.sum(jnp.where(lane == TOK, total_masked, 0.0), axis=1, keepdims=True)
    mean = total_masked / jnp.maximum(started_count, 1.0)
    mean_ref[...] = jnp.broadcast_to(mean, (1, 128))
    mine_s = z * NY + y
    index = jnp.where(z < NZ // 2, mine_s, 31 - mine_s)
    dz = lax.rem(index // 2 + NZ // 2 - z + NZ, NZ)
    other = jnp.where(z < NZ // 2, c, 1 - c)
    ent_ref[...] = ents[dz * 2 + other, lax.rem(index, 2)][:, 0:TOK]
    all_ents.wait_send()


def local(hidden, lm_head, positions, vocab_limits, loss_mask):
    f32, bf16 = jnp.float32, jnp.bfloat16
    dma = pltpu.SemaphoreType.DMA
    any_space = pl.BlockSpec(memory_space=pl.ANY)
    vmem = pl.BlockSpec(memory_space=pltpu.VMEM)
    ent, mean = pl.pallas_call(
        kernel,
        out_shape=(jax.ShapeDtypeStruct((1, TOK), f32), jax.ShapeDtypeStruct((1, 128), f32)),
        in_specs=[any_space] * 5,
        out_specs=(vmem, vmem),
        scratch_shapes=[
            pltpu.VMEM((NZ * COLORS * CHUNK, D), bf16),
            pltpu.VMEM((2, PAD, D), bf16),
            pltpu.VMEM((2, WID, D), bf16),
            pltpu.VMEM((TOK, FEAT // 2), bf16),
            pltpu.VMEM((HALF, FEAT // 2), bf16),
            pltpu.VMEM((2, 2, PAD, LANES), f32),
            pltpu.VMEM((2, 24, 128), jnp.int32),
            pltpu.VMEM((1, TOK), jnp.int32),
            pltpu.VMEM((2, NZ, LANES), f32),
            pltpu.VMEM((WINDOWS, 1, LANES), jnp.int32),
            pltpu.VMEM((LANES, 128), f32),
            pltpu.VMEM((WINDOWS, 8, LANES), f32),
            pltpu.VMEM((NZ, 3, 1, 256), f32),
            pltpu.VMEM((NZ, 3, 1, 256), f32),
            pltpu.VMEM((3, 1, 256), f32),
            pltpu.VMEM((NY * NX, 3, 1, 256), f32),
            pltpu.VMEM((2 * NZ, 2, 1, 128), f32),
            pltpu.VMEM((NZ, NY, 1, 128), f32),
            dma((2 + len(SMALL) - WHOLE,)), dma((SEMAPHORES,)), *[dma((2,))] * 7, dma((5,)),
        ],
        compiler_params=pltpu.CompilerParams(
            collective_id=0, has_side_effects=True, vmem_limit_bytes=62 * 2**20),
    )(hidden, lm_head.T, positions.reshape(24, 128), vocab_limits.reshape(24, 128), loss_mask.reshape(1, TOK))
    return ent.reshape(TOK), mean[0, 0]


def solution(mesh):
    torus = Mesh(mesh.devices.reshape(NZ, NY, NX, 2), AXES)
    in_specs = (P(("z", "y"), ("x", "c")), P(None, AXES), P(), P(), P(("z", "y")))
    return jax.shard_map(local, mesh=torus, in_specs=in_specs, out_specs=(P(("z", "y")), P()), check_vma=False)
```

```python
import heapq

import jax
import jax.numpy as jnp
from jax import lax
from jax.experimental import pallas as pl
from jax.experimental.pallas import tpu as pltpu
from jax.sharding import Mesh
from jax.sharding import PartitionSpec as P

NZ, NY, NX = 8, 4, 4
SIZE = {"z": NZ, "y": NY, "x": NX}
AXES = ("z", "y", "x", "c")
MESH = pl.DeviceIdType.MESH
HALF, RB, COLORS = 48, 16, 3
TOK = 96
D, FEAT = 3584, 896
WID, PAD = 594, 608
CHUNK, LANES = 64, 256
WINDOWS = NZ * COLORS * CHUNK // LANES
NEG = -1e30
DEADLINE = (
    (-18.7, -45.5, 48.4),
    (-28.8, 7.7, -36.2),
    (72.7, 12.8, 9.8),
    (-33.4, 28.9, 15.4),
    (-4.9, 31.5, 18.3),
    (10.5, 12.3, -3.5),
    (-36.7, 12.9, 18.2),
    (79.1, 7.0, 5.2),
)
UNIT, HOP, BACKLOG = 0.615, 2.5, 1.5
DEEP = 3.5
WINDOW = 3.05


def onward(n, d, far):
    if d == 0:
        return [1, -1]
    if d < n // 2:
        return [-1] if d + 1 < n // 2 or far == -1 else []
    if d > n // 2:
        return [1] if d - 1 > n // 2 or far == 1 else []
    return []


def parity(k):
    return 1 if k % 2 == 0 else -1


def sends_of(p):
    color, axis, rest = p[0], p[1], p[2:]
    out = []
    if color == "A" and axis == "y":
        (dy,) = rest
        out += [("y", m, 1, ("A", "y", (dy - m) % 4)) for m in onward(4, dy, 1)]
        out += [("x", m, 1, ("A", "x", dy, -m % 4)) for m in (1, -1)]
    elif color == "A" and axis == "x":
        dy, dx = rest
        out += [("x", m, 1, ("A", "x", dy, (dx - m) % 4)) for m in onward(4, dx, parity(dy))]
    elif color == "A":
        dz, dy = rest
        out += [("z", m, 4, ("A", "z", (dz - m) % 8, dy)) for m in onward(8, dz, parity(dy))]
    elif axis == "z":
        (dz,) = rest
        far = 1 if color == "B" else -1
        out += [("z", m, 1, (color, "z", (dz - m) % 8)) for m in onward(8, dz, far)]
        second = "y" if color == "B" else "x"
        out += [(second, m, 1, (color, second, dz, -m % 4)) for m in (1, -1)]
    else:
        dz, d = rest
        last = (color, axis) in (("B", "x"), ("C", "y"))
        size = 4 if last else 1
        out += [(axis, m, size, (color, axis, dz, (d - m) % 4)) for m in onward(4, d, parity(dz))]
    return out


def launch_of(p):
    color, axis = p[0], p[1]
    if color == "A" and axis != "z":
        return ("A", "z", 0, p[2])
    if color == "B" and axis != "x":
        return ("B", "x", p[2], 0)
    if color == "C" and axis != "y":
        return ("C", "y", p[2], 0)
    return None


def parts_of(launch):
    color, _, a, b = launch
    if color == "A":
        return [("A", "y", b)] + [("A", "x", b, k) for k in (1, 2, 3)]
    if color == "B":
        return [("B", "z", a)] + [("B", "y", a, k) for k in (1, 2, 3)]
    return [("C", "z", a)] + [("C", "x", a, k) for k in (1, 2, 3)]


def window_of(p):
    return 0 if p[0] == "A" and p[1] != "z" else p[2]


def pieces_of_chunk(dz, color):
    last = (("A", "z"), ("B", "x"), ("C", "y"))[color]
    return [(*last, dz, k) for k in range(4)]


def plan(preps, chunks=None):
    due = {}

    def latest(p):
        if p not in due:
            dz = window_of(p)
            k = DEADLINE[dz][{"A": 0, "B": 1, "C": 2}[p[0]]]
            ahead = sends_of(p)
            launch = launch_of(p)
            if launch:
                ahead = ahead + sends_of(launch)
            for _, _, size, q in ahead:
                k = min(k, latest(q) - HOP - size * UNIT - 0.3)
            due[p] = k
        return due[p]

    free = {(a, m): 0.0 for a in "xyz" for m in (1, -1)}
    waiting = {k: [] for k in free}
    have, steps, flying = set(), [], []
    count = 0
    now = 0.0

    def offer(sends):
        nonlocal count
        for axis, m, size, q in sends:
            heapq.heappush(waiting[axis, m], (latest(q) - size * UNIT, count, size, q))
            count += 1

    def pump(ahead=None):
        nonlocal count
        ahead = BACKLOG if ahead is None else ahead
        for link in free:
            while waiting[link] and free[link] - now < ahead:
                _, _, size, q = heapq.heappop(waiting[link])
                free[link] = max(free[link], now) + size * UNIT
                heapq.heappush(flying, (free[link] + HOP, count, q))
                count += 1
                steps.append(("send", link[0], link[1], q))

    def take(p):
        have.add(p)
        offer(sends_of(p))
        launch = launch_of(p)
        if launch and launch not in have and all(q in have for q in parts_of(launch)):
            have.add(launch)
            offer(sends_of(launch))

    def blocked():
        return any(p[0][0] == "other" for p in preps)

    for p in (("A", "y", 0), ("B", "z", 0), ("C", "z", 0)):
        take(p)
    pump()
    arrived = {}
    left = list(range(WINDOWS)) if chunks else []
    preps = list(preps)
    while flying or left or preps:
        if flying and flying[0][0] <= now:
            _, _, q = heapq.heappop(flying)
            steps.append(("wait", q))
            arrived[q] = now
            take(q)
            pump()
            now += 0.03
            continue
        if preps and now >= preps[0][1]:
            name, _, cost = preps.pop(0)
            steps.append(("prep", name))
            now += cost
            pump()
            continue
        ready = [] if blocked() else [w for w in left if all(
            q in have for chunk in chunks[4 * w:4 * w + 4] for q in pieces_of_chunk(*chunk))]
        if ready:
            pump(DEEP)
            steps.append(("window", ready[0]))
            left.remove(ready[0])
            now += WINDOW
            pump()
            continue
        nxt = [flying[0][0]] if flying else []
        if preps:
            nxt.append(preps[0][1])
        now = max(now, min(nxt))
    if chunks is None:
        every = [(dz, color) for dz in range(NZ) for color in range(COLORS)]
        return sorted(every, key=lambda t: max(arrived.get(q, 0.0) for q in pieces_of_chunk(*t)))
    return steps, now


PREPS = (
    [(("limits", 0), 0.2, 0.3), (("places", 0), 0.8, 0.4)]
    + [(("own", k), 3.0, 0.3) for k in range(2)]
    + [(("other", k), 11.0, 0.3) for k in range(2)]
    + [(("mask", 0), 16.0, 0.1), (("mask", 1), 32.0, 0.1)]
)
CHUNKS = plan(PREPS)
STEPS, _ = plan(PREPS, CHUNKS)
SPOT = {chunk: k for k, chunk in enumerate(CHUNKS)}
TRANSFERS = [s[3] for s in STEPS if s[0] == "send"]


def shared_semaphores(steps):
    sent = {s[3]: k for k, s in enumerate(steps) if s[0] == "send"}
    waited = {s[1]: k for k, s in enumerate(steps) if s[0] == "wait"}
    links = {}
    for s in steps:
        if s[0] == "send":
            links.setdefault(s[1:3], []).append(s[3])
    number, count = {}, 0
    for (axis, m), queue in links.items():
        slots = []
        for q in queue:
            for slot in slots:
                if any(sent[r] > waited[slot[1]] and waited[r] < sent[q] for r in links[axis, -m]):
                    break
            else:
                slot = [count, None]
                slots.append(slot)
                count += 1
            slot[1] = q
            number[q] = slot[0]
    return number, count


NUMBER, SEMAPHORES = shared_semaphores(STEPS)
LARGE = [q for q in TRANSFERS if q[:2] in (("A", "z"), ("B", "x"), ("C", "y"))]
SMALL = [q for q in TRANSFERS if q not in LARGE]
WHOLE = len(SMALL) // 4 * 4
GROUP = {q: 0 for q in LARGE}
GROUP.update({q: 1 if k < WHOLE else 2 + k - WHOLE for k, q in enumerate(SMALL)})


def merge(parts):
    peak = parts[0][0]
    for p in parts[1:]:
        peak = jnp.maximum(peak, p[0])
    total = jnp.zeros_like(peak)
    moment = jnp.zeros_like(peak)
    for m, t, mo in parts:
        shift = m - peak
        ratio = jnp.exp(shift)
        total = total + ratio * t
        moment = moment + ratio * (mo + t * shift)
    return peak, total, moment


def kernel(hid_ref, lm_ref, pos_ref, lim_ref, mask_ref, ent_ref, mean_ref,
           held, weight, stage, hstage, pstage, logits, small, mask_in, table, lim_win, pos_col,
           wstat, stat, from_z, plane, from_plane, ents, masks,
           send_sem, recv_sem, hx_sem, w_sem, mz_sem, my_sem, rz_sem, rp_sem, re_sem, copy_sem):
    z, y, x, c = (lax.axis_index(a) for a in AXES)
    here = {"z": z, "y": y, "x": x, "c": c}

    def device(**moved):
        return tuple(lax.rem(here[a] + moved[a], SIZE[a]) if a in moved and a != "c" else
                     (1 - c if a in moved else here[a]) for a in AXES)

    own_w = pltpu.make_async_copy(lm_ref, stage.at[0], copy_sem.at[0])
    own_h = pltpu.make_async_copy(hid_ref, hstage, copy_sem.at[1])
    own_h.start()
    own_w.start()
    given = [pltpu.make_async_copy(lim_ref, small.at[0], copy_sem.at[2]),
             pltpu.make_async_copy(pos_ref, small.at[1], copy_sem.at[3]),
             pltpu.make_async_copy(mask_ref, mask_in, copy_sem.at[4])]
    for copy in given:
        copy.start()

    barrier = pltpu.get_barrier_semaphore()
    near = [device(**{a: d}) for a in "zyx" for d in (1, SIZE[a] - 1)] + [device(c=1)]
    for who in near:
        pl.semaphore_signal(barrier, inc=1, device_id=who, device_id_type=MESH)
    with jax.named_scope("T_barrier"):
        pl.semaphore_wait(barrier, len(near))

    with jax.named_scope("T_ownh"):
        own_h.wait()
    swap = pltpu.make_async_remote_copy(
        src_ref=hstage.at[pl.ds(pl.multiple_of((1 - c) * HALF, RB), HALF), :], dst_ref=pstage,
        send_sem=hx_sem.at[0], recv_sem=hx_sem.at[1], device_id=device(c=1), device_id_type=MESH)
    swap.start()
    give_w = pltpu.make_async_remote_copy(
        src_ref=lm_ref, dst_ref=stage.at[1],
        send_sem=w_sem.at[0], recv_sem=w_sem.at[1], device_id=device(c=1), device_id_type=MESH)
    give_w.start()

    def feature(dx):
        return pl.ds(pl.multiple_of(lax.rem(x + dx, NX) * FEAT, 128), FEAT)

    mine = hstage[pl.ds(pl.multiple_of(c * HALF, RB), HALF), :].astype(jnp.float32)
    with jax.named_scope("T_swap"):
        swap.wait_recv()
    theirs = pstage[...].astype(jnp.float32)
    first = c == 0
    left = jnp.where(first, mine, theirs)
    right = jnp.where(first, theirs, mine)
    both = jnp.concatenate([left, right], axis=1).astype(jnp.bfloat16)
    for k in range(COLORS):
        held[pl.ds(SPOT[0, k] * CHUNK, RB), feature(0)] = both[k * RB:(k + 1) * RB]

    def rows_of(p):
        color, axis = "ABC".index(p[0]), p[1]
        dz = window_of(p)
        if p[:2] == ("B", "x"):
            return pl.ds(SPOT[dz, color] * CHUNK, CHUNK)
        if axis == "z":
            dy = p[3] if color == 0 else 0
        elif axis == "y":
            dy = p[2] if color == 0 else p[3]
        else:
            dy = p[2] if color == 0 else 0
        return pl.ds(SPOT[dz, color] * CHUNK + dy * RB, RB)

    def place(p):
        if p[:2] in (("A", "z"), ("C", "y")):
            return held.at[rows_of(p), :]
        return held.at[rows_of(p), feature(p[-1] if p[1] == "x" else 0)]

    def transfer(q, axis, m):
        n = SIZE[axis]
        if axis == "x":
            src = dst = held.at[rows_of(q), feature(q[-1] + m + NX)]
        else:
            at = {("A", "y"): 2, ("A", "z"): 2, ("B", "z"): 2, ("C", "z"): 2}.get(q[:2], 3)
            src = place(q[:at] + ((q[at] + m) % n,) + q[at + 1:])
            dst = place(q)
        return pltpu.make_async_remote_copy(
            src_ref=src, dst_ref=dst, send_sem=send_sem.at[GROUP[q]], recv_sem=recv_sem.at[NUMBER[q]],
            device_id=device(**{axis: m % n}), device_id_type=MESH)

    started = {}
    lanes = lax.broadcasted_iota(jnp.int32, (128, 128), 1)

    rows_z = lax.rem(z + NZ // 2, NZ)
    lane_of = lax.broadcasted_iota(jnp.int32, (8, LANES), 1)
    lane_chunk = lane_of // CHUNK

    def limits():
        for copy in given:
            copy.wait()
        masks[0, 0] = jnp.zeros((1, 128), jnp.float32)
        masks[0, 0, :, 0:TOK] = mask_in[...].astype(jnp.float32)
        row = lax.broadcasted_iota(jnp.int32, (3 * 128, LANES), 0)
        column = lax.broadcasted_iota(jnp.int32, (3 * 128, LANES), 1)
        color, dy, i = column // CHUNK, column % CHUNK // RB, column % RB
        want = lax.rem(y + dy, NY) * TOK + c * HALF + color * RB + i
        pick = jnp.where((row == want) & (color < COLORS), 1.0, 0.0).astype(jnp.bfloat16)
        for k in range(2):
            given_rows = jnp.concatenate(
                [small[k, pl.ds(j, NZ, stride=3), :] for j in range(3)], axis=1)
            found = jnp.zeros((NZ, LANES), jnp.float32)
            for shift in (14, 7, 0):
                digit = lax.bitwise_and(lax.shift_right_logical(given_rows, shift), 127)
                digit = digit.astype(jnp.float32).astype(jnp.bfloat16)
                found = found * 128.0 + jnp.dot(digit, pick, preferred_element_type=jnp.float32)
            table[k] = found

    def places():
        for w in range(WINDOWS):
            line = jnp.zeros((8, LANES), jnp.float32)
            for j in range(4):
                dz, color = CHUNKS[4 * w + j]
                source = jnp.broadcast_to(table[0, pl.ds(lax.rem(z + dz, NZ), 1), :], (8, LANES))
                if j != color:
                    source = pltpu.roll(source, (j - color) * CHUNK % LANES, 1)
                line = jnp.where(lane_chunk == j, source, line)
            lim_win[w] = line[0:1].astype(jnp.int32)
        pos_col[...] = jnp.broadcast_to(table[1, pl.ds(rows_z, 1), :], (128, LANES)).T

    def settle(which, k):
        def one(r, carry):
            at = pl.ds(pl.multiple_of(r * 256, 128), 256)
            weight[which, 0:WID, at] = stage[which, :, at]
            return carry

        lax.fori_loop(7 * k, 7 * k + 7, one, 0)

    def mask_z(dz):
        return pltpu.make_async_remote_copy(
            src_ref=masks.at[0, 0], dst_ref=masks.at[8 - dz, 0], send_sem=mz_sem.at[0],
            recv_sem=mz_sem.at[1], device_id=device(z=dz), device_id_type=MESH)

    def mask_y(dy):
        return pltpu.make_async_remote_copy(
            src_ref=masks.at[:, 0], dst_ref=masks.at[:, 4 - dy], send_sem=my_sem.at[0],
            recv_sem=my_sem.at[1], device_id=device(y=dy), device_id_type=MESH)

    def whole(ref, sems):
        return pltpu.make_async_remote_copy(
            src_ref=ref, dst_ref=ref, send_sem=sems.at[0], recv_sem=sems.at[1],
            device_id=device(z=1), device_id_type=MESH)

    all_mask_z = whole(masks.at[1:NZ, 0], mz_sem)
    all_mask_y = whole(masks.at[:, 1:NY], my_sem)
    all_stat = whole(from_z.at[1:NZ], rz_sem)
    all_plane = whole(from_plane.at[1:NY * NX], rp_sem)
    all_ents = whole(ents.at[1:2 * NZ], re_sem)

    def prep(name, k):
        if name == "limits":
            limits()
        elif name == "places":
            places()
        elif name == "own":
            if k == 0:
                own_w.wait()
            settle(0, k)
        elif name == "other":
            if k == 0:
                give_w.wait_recv()
            settle(1, k)
        elif k == 0:
            for dz in range(1, NZ):
                mask_z(dz).start()
        else:
            all_mask_z.wait_recv()
            for dy in range(1, NY):
                mask_y(dy).start()

    number = (z * NY + y) * (2 * NX) + x * 2
    starts = ((number + c) * WID, (number + 1 - c) * WID)
    depth = lax.broadcasted_iota(jnp.int32, (PAD, LANES), 0)

    def multiply(w, slot):
        for k in range(2):
            logits[slot, k] = lax.dot_general(
                weight[k], held[w * LANES:(w + 1) * LANES, :], (((1,), (1,)), ((), ())),
                preferred_element_type=jnp.float32)

    def reduce_rows(w, slot):
        limit = lim_win[w]
        peak = jnp.full((1, LANES), NEG, jnp.float32)
        for k in range(2):
            bound = jnp.minimum(limit - starts[k], WID)
            allowed = jnp.where(depth < bound, logits[slot, k], NEG)
            peak = jnp.maximum(peak, jnp.max(allowed, axis=0, keepdims=True))
        total = jnp.zeros((1, LANES), jnp.float32)
        moment = jnp.zeros((1, LANES), jnp.float32)
        for k in range(2):
            bound = jnp.minimum(limit - starts[k], WID)
            shifted = jnp.where(depth < bound, logits[slot, k], NEG) - peak
            e = jnp.exp(shifted)
            total = total + jnp.sum(e, axis=0, keepdims=True)
            moment = moment + jnp.sum(e * shifted, axis=0, keepdims=True)
        wstat[w] = jnp.concatenate([peak, total, moment, jnp.zeros((5, LANES), jnp.float32)], axis=0)
        reduced.append(w)
        for dz in range(NZ):
            spots = [SPOT[dz, color] for color in range(COLORS)]
            if any(spot // 4 == w for spot in spots) and all(spot // 4 in reduced for spot in spots):
                line = jnp.zeros((8, LANES), jnp.float32)
                for color, spot in enumerate(spots):
                    source = wstat[spot // 4]
                    if spot % 4 != color:
                        source = pltpu.roll(source, (color - spot % 4) * CHUNK % LANES, 1)
                    line = jnp.where(lane_chunk == color, source, line)
                for k in range(3):
                    stat[dz, k] = line[k:k + 1]
                if dz != NZ // 2:
                    stat_copy(dz).start()

    def stat_copy(dz):
        ahead = (dz + NZ // 2) % NZ
        return pltpu.make_async_remote_copy(
            src_ref=stat.at[dz], dst_ref=from_z.at[NZ - ahead], send_sem=rz_sem.at[0],
            recv_sem=rz_sem.at[1], device_id=device(z=ahead), device_id_type=MESH)

    done, reduced = [], []

    def window(dz):
        if done:
            reduce_rows(done[-1], len(done) % 2)
        if dz is None:
            return
        done.append(dz)
        multiply(dz, len(done) % 2)

    for step in STEPS:
        if step[0] == "send":
            _, axis, m, q = step
            started[q] = transfer(q, axis, m)
            started[q].start()
        else:
            if step[0] == "wait":
                started[step[1]].wait_recv()
            elif step[0] == "prep":
                prep(*step[1])
            else:
                window(step[1])
    with jax.named_scope("T_last"):
        window(None)

    with jax.named_scope("T_zround"):
        all_stat.wait_recv()
    parts = [tuple(stat[NZ // 2, k] for k in range(3))]
    parts += [tuple(from_z[dz, k] for k in range(3)) for dz in range(1, NZ)]
    merged = merge(parts)
    for k in range(3):
        plane[k] = merged[k]

    spots = [(dy, dx) for dy in range(NY) for dx in range(NX) if dy or dx]

    def plane_copy(dy, dx):
        back = (NY - dy) % NY * NX + (NX - dx) % NX
        return pltpu.make_async_remote_copy(
            src_ref=plane, dst_ref=from_plane.at[back], send_sem=rp_sem.at[0],
            recv_sem=rp_sem.at[1], device_id=device(y=dy, x=dx), device_id_type=MESH)

    for dy, dx in spots:
        plane_copy(dy, dx).start()
    all_mask_y.wait_recv()
    with jax.named_scope("T_planeround"):
        all_plane.wait_recv()
    groups = []
    for dy in range(NY):
        parts = [tuple(from_plane[dy * NX + dx, k] for k in range(3)) for dx in range(NX) if dy or dx]
        group = merge(parts if dy else [merged] + parts)
        if dy:
            lines = jnp.concatenate([*group, jnp.zeros((5, LANES), jnp.float32)], axis=0)
            ahead = pltpu.roll(lines, dy * RB, 1)
            around = pltpu.roll(lines, (dy * RB - CHUNK) % LANES, 1)
            lines = jnp.where(lane_of % CHUNK >= dy * RB, ahead, around)
            group = tuple(lines[k:k + 1] for k in range(3))
        groups.append(group)
    peak, total, moment = merge(groups)
    entropy = jnp.log(total) - moment / total

    masked = jnp.zeros((1, 128), jnp.float32)
    found = []
    column = jnp.broadcast_to(entropy, (128, LANES)).T[:COLORS * CHUNK]
    for k in range(2):
        owner = jnp.where(c == 0, 2 * rows_z + k, 31 - 2 * rows_z - k)
        line = lanes[:1]
        spot = jnp.where(line < TOK, owner * TOK + line, -1).astype(jnp.float32)
        here_e = jnp.where(pos_col[0:COLORS * CHUNK, :] == spot, column, 0.0)
        here_e = jnp.sum(here_e, axis=0, keepdims=True)
        found.append(here_e)
        dz = lax.rem(owner // NY - z + NZ, NZ)
        dy = lax.rem(lax.rem(owner, NY) - y + NY, NY)
        masked = masked + here_e * masks[dz, dy]
    masked = jnp.sum(masked, axis=1, keepdims=True)
    lane = lanes[:1]
    for k in range(2):
        ents[0, k] = jnp.where(lane < TOK, found[k], masked if k == 0 else 0.0)

    others = [(dz, other) for dz in range(NZ) for other in range(2) if dz or other]

    def ent_copy(dz, other):
        target = device(z=dz, c=1) if other else device(z=dz)
        return pltpu.make_async_remote_copy(
            src_ref=ents.at[0], dst_ref=ents.at[(NZ - dz) % NZ * 2 + other], send_sem=re_sem.at[0],
            recv_sem=re_sem.at[1], device_id=target, device_id_type=MESH)

    for dz, other in others:
        ent_copy(dz, other).start()

    started_count = jnp.sum(jnp.sum(masks[...].reshape(NZ * NY, 128), axis=0, keepdims=True), axis=1, keepdims=True)
    for group, rows in ((0, len(LARGE) * RB), (1, WHOLE // 4 * RB)):
        pltpu.make_async_remote_copy(
            src_ref=held.at[0:rows, :], dst_ref=held.at[0:rows, :], send_sem=send_sem.at[group],
            recv_sem=recv_sem.at[0], device_id=device(z=1), device_id_type=MESH).wait_send()
    for q in SMALL[WHOLE:]:
        started[q].wait_send()
    swap.wait_send()
    give_w.wait_send()
    all_mask_z.wait_send()
    all_mask_y.wait_send()
    all_stat.wait_send()
    all_plane.wait_send()

    with jax.named_scope("T_entround"):
        all_ents.wait_recv()
    total_masked = jnp.sum(ents[:, 0].reshape(2 * NZ, 128), axis=0, keepdims=True)
    total_masked = jnp.sum(jnp.where(lane == TOK, total_masked, 0.0), axis=1, keepdims=True)
    mean = total_masked / jnp.maximum(started_count, 1.0)
    mean_ref[...] = jnp.broadcast_to(mean, (1, 128))
    mine_s = z * NY + y
    index = jnp.where(z < NZ // 2, mine_s, 31 - mine_s)
    dz = lax.rem(index // 2 + NZ // 2 - z + NZ, NZ)
    other = jnp.where(z < NZ // 2, c, 1 - c)
    ent_ref[...] = ents[dz * 2 + other, lax.rem(index, 2)][:, 0:TOK]
    all_ents.wait_send()


def local(hidden, lm_head, positions, vocab_limits, loss_mask):
    f32, bf16 = jnp.float32, jnp.bfloat16
    dma = pltpu.SemaphoreType.DMA
    any_space = pl.BlockSpec(memory_space=pl.ANY)
    vmem = pl.BlockSpec(memory_space=pltpu.VMEM)
    ent, mean = pl.pallas_call(
        kernel,
        out_shape=(jax.ShapeDtypeStruct((1, TOK), f32), jax.ShapeDtypeStruct((1, 128), f32)),
        in_specs=[any_space] * 5,
        out_specs=(vmem, vmem),
        scratch_shapes=[
            pltpu.VMEM((NZ * COLORS * CHUNK, D), bf16),
            pltpu.VMEM((2, PAD, D), bf16),
            pltpu.VMEM((2, WID, D), bf16),
            pltpu.VMEM((TOK, FEAT // 2), bf16),
            pltpu.VMEM((HALF, FEAT // 2), bf16),
            pltpu.VMEM((2, 2, PAD, LANES), f32),
            pltpu.VMEM((2, 24, 128), jnp.int32),
            pltpu.VMEM((1, TOK), jnp.int32),
            pltpu.VMEM((2, NZ, LANES), f32),
            pltpu.VMEM((WINDOWS, 1, LANES), jnp.int32),
            pltpu.VMEM((LANES, 128), f32),
            pltpu.VMEM((WINDOWS, 8, LANES), f32),
            pltpu.VMEM((NZ, 3, 1, 256), f32),
            pltpu.VMEM((NZ, 3, 1, 256), f32),
            pltpu.VMEM((3, 1, 256), f32),
            pltpu.VMEM((NY * NX, 3, 1, 256), f32),
            pltpu.VMEM((2 * NZ, 2, 1, 128), f32),
            pltpu.VMEM((NZ, NY, 1, 128), f32),
            dma((2 + len(SMALL) - WHOLE,)), dma((SEMAPHORES,)), *[dma((2,))] * 7, dma((5,)),
        ],
        compiler_params=pltpu.CompilerParams(
            collective_id=0, has_side_effects=True, vmem_limit_bytes=62 * 2**20),
    )(hidden, lm_head.T, positions.reshape(24, 128), vocab_limits.reshape(24, 128), loss_mask.reshape(1, TOK))
    return ent.reshape(TOK), mean[0, 0]


def solution(mesh):
    torus = Mesh(mesh.devices.reshape(NZ, NY, NX, 2), AXES)
    in_specs = (P(("z", "y"), ("x", "c")), P(None, AXES), P(), P(), P(("z", "y")))
    return jax.shard_map(local, mesh=torus, in_specs=in_specs, out_specs=(P(("z", "y")), P()), check_vma=False)
```
